128 devices in a mesh: gx: 16 (over z, y), gy: 8 (over x, core).
Axes of the slice: x: 4, y: 4, z: 4, core: 2. Of those that a mesh axis runs over, the one named last changes fastest.
Arguments:
- fine_nodes: bfloat16 [131072, 512], P(('gx', 'gy')), may hold values from -6 to 6
- edge_latent: bfloat16 [786432, 512], P(('gx', 'gy')), may hold values from -6 to 6
- boundary: int32 [16384], P(('gx', 'gy')), may hold values from 0 to 1023, as said below
- fine_src: int32 [786432], P(('gx', 'gy')), may hold values from 0 to 2175, as said below
- fine_dst: int32 [786432], P(('gx', 'gy')), may hold values from 0 to 1023
- parent_one: int32 [131072], P(('gx', 'gy')), may hold values from 0 to 831, as said below
- weight_one: bfloat16 [131072], P(('gx', 'gy')), may hold values from 0.049804688 to 0.29882812
- coarse_src_one: int32 [196608], P(('gx', 'gy')), may hold values from 0 to 831, as said below
- coarse_dst_one: int32 [196608], P(('gx', 'gy')), may hold values from 0 to 255
- parent_two: int32 [32768], P(('gx', 'gy')), may hold values from 0 to 351, as said below
- weight_two: bfloat16 [32768], P(('gx', 'gy')), may hold values from 0.099609375 to 0.5
- coarse_src_two: int32 [49152], P(('gx', 'gy')), may hold values from 0 to 351, as said below
- coarse_dst_two: int32 [49152], P(('gx', 'gy')), may hold values from 0 to 63
- fine_message_in: bfloat16 [1536, 512], replicated, may hold values from -0.15625 to 0.15625
- fine_message_out: bfloat16 [512, 512], replicated, may hold values from -0.25 to 0.25
- fine_message_gain: bfloat16 [512], replicated, may hold values from 0.25 to 1.75
- fine_update_in: bfloat16 [1024, 512], replicated, may hold values from -0.1875 to 0.1875
- fine_update_out: bfloat16 [512, 512], replicated, may hold values from -0.25 to 0.25
- fine_update_gain: bfloat16 [512], replicated, may hold values from 0.25 to 1.75
- coarse_message_in: bfloat16 [1024, 512], replicated, may hold values from -0.1875 to 0.1875
- coarse_message_out: bfloat16 [512, 512], replicated, may hold values from -0.25 to 0.25
- coarse_message_gain: bfloat16 [512], replicated, may hold values from 0.25 to 1.75
- coarse_update_in: bfloat16 [1024, 512], replicated, may hold values from -0.1875 to 0.1875
- coarse_update_out: bfloat16 [512, 512], replicated, may hold values from -0.25 to 0.25
- coarse_update_gain: bfloat16 [512], replicated, may hold values from 0.25 to 1.75
Outputs:
- fine_out: bfloat16 [131072, 512], P(('gx', 'gy'))
The draws below stay inside these ranges and needn't reach their ends.
Inputs may be any that keep to these rules, and one draw needn't show every extreme that they name: `boundary`: each device's 128 entries are distinct local row numbers of its own fine nodes. `fine_src`: an entry below 1024 is a local row of the edge's own device; an entry 1024 + k * 128 + r names boundary row r of the device at grid offset (k // 3 - 1, k % 3 - 1) along (gx, gy), with wrap; k is never 4. `parent_one`: an entry below 256 is a first coarse level row of the fine node's own device; an entry 256 + k * 64 + r names rim row r of the device at grid offset (k // 3 - 1, k % 3 - 1) along (gx, gy), with wrap; k is never 4. `coarse_src_one`: an entry below 256 is a first coarse level row of the edge's own device; an entry 256 + k * 64 + r names rim row r of the device at grid offset (k // 3 - 1, k % 3 - 1) along (gx, gy), with wrap; k is never 4. `parent_two`: an entry below 64 is a second coarse level row of the node's own device; an entry 64 + k * 32 + r names rim row r of the device at grid offset (k // 3 - 1, k % 3 - 1) along (gx, gy), with wrap; k is never 4. `coarse_src_two`: an entry below 64 is a second coarse level row of the edge's own device; an entry 64 + k * 32 + r names rim row r of the device at grid offset (k // 3 - 1, k % 3 - 1) along (gx, gy), with wrap; k is never 4.
All inputs are finite; a program needn't handle non-finite values.
Results may differ from the reference program's by a relative error of at most 0.012.
Values may be sent and summed in bfloat16 or wider, within the bound.
A program may use at most 128 MiB of HBM per device.

```python
import math
import jax
import jax.numpy as jnp
from jax import lax

D = 512
NF_DEV = 1024
BND = 128
E_DEV = 6144
NC1_DEV = 256
NC2_DEV = 64
CB1 = 64
CB2 = 32
E1_DEV = 1536
E2_DEV = 384
NF = 131072
NC1 = 32768
NC2 = 8192
N_GX = 16
N_GY = 8


def rim_numbers(key, count, local_count, rim_count, outward):
    streams = jax.random.split(key, 4)
    inside = jax.random.randint(streams[0], (count,), 0, local_count)
    sector = jax.random.randint(streams[1], (count,), 0, 8)
    sector = sector + (sector >= 4).astype(jnp.int32)
    beyond = local_count + sector * rim_count + jax.random.randint(streams[2], (count,), 0, rim_count)
    chosen = jax.random.randint(streams[3], (count,), 0, 8) < outward
    return jnp.where(chosen, beyond, inside).astype(jnp.int32)


def draw_boundary(key, part):
    scores = jax.random.randint(jax.random.fold_in(key, 11), (N_GX * N_GY, NF_DEV), 0, 65536)
    scores = scores * NF_DEV + jnp.arange(NF_DEV, dtype=jnp.int32)[None, :]
    ordering = jnp.argsort(scores, axis=1)
    return ordering[:, :BND].reshape(-1).astype(jnp.int32)


def draw_fine_src(key, part):
    return rim_numbers(jax.random.fold_in(key, 23), N_GX * N_GY * E_DEV, NF_DEV, BND, 4)


def draw_parent_one(key, part):
    return rim_numbers(jax.random.fold_in(key, 31), N_GX * N_GY * NF_DEV, NC1_DEV, CB1, 4)


def draw_coarse_src_one(key, part):
    return rim_numbers(jax.random.fold_in(key, 37), N_GX * N_GY * E1_DEV, NC1_DEV, CB1, 4)


def draw_parent_two(key, part):
    return rim_numbers(jax.random.fold_in(key, 41), N_GX * N_GY * NC1_DEV, NC2_DEV, CB2, 5)


def draw_coarse_src_two(key, part):
    return rim_numbers(jax.random.fold_in(key, 43), N_GX * N_GY * E2_DEV, NC2_DEV, CB2, 4)


def touch_ends(result, own_key, least, high):
    longest = result.shape.index(max(result.shape))
    spots = []
    for shift in (0, 1):
        where = [jax.random.randint(jax.random.fold_in(own_key, axis), (), 0, length) for axis, length in enumerate(result.shape)]
        where[longest] = (where[longest] + shift) % result.shape[longest]
        spots.append(tuple(where))
    return result.at[spots[0]].set(least).at[spots[1]].set(high)


def steps_of(key, extent, shards, low, top_value):
    factor_of, own = 1.0, jax.random.fold_in(key, 6)
    for dim, shards_of in shards:
        heights = jnp.exp(jax.random.uniform(jax.random.fold_in(own, dim), (shards_of,), jnp.float32, low / len(shards), top_value / len(shards)))
        factor_of = factor_of * jnp.repeat(heights, extent[dim] // shards_of).reshape([-1 if axis == dim else 1 for axis in range(len(extent))])
    return factor_of


def normal_values(rng, dims, width, reach, cuts=(), held_as=jnp.bfloat16):
    factor_of = steps_of(rng, dims, cuts, -0.22, 0.18) if cuts else 1.0
    result = jax.random.normal(rng, dims, jnp.float32) * width * factor_of
    return jnp.minimum(jnp.maximum(result, -reach), reach).astype(held_as)


def setup_inputs(seed: int = 0) -> dict:
    seeds = jax.random.split(jax.random.key(seed), 26)
    fine_nodes = normal_values(seeds[0], (NF, D), 1.0, 6.0, ((0, 128),))
    edge_latent = normal_values(seeds[1], (N_GX * N_GY * E_DEV, D), 1.0, 6.0, ((0, 128),))
    boundary = draw_boundary(jax.random.fold_in(seeds[25], 71), 0)
    fine_src = draw_fine_src(jax.random.fold_in(seeds[25], 71), 0)
    fine_dst = touch_ends(jax.random.randint(seeds[4], (N_GX * N_GY * E_DEV,), 0, NF_DEV), jax.random.fold_in(seeds[4], 1), 0, NF_DEV - 1).astype(jnp.int32)
    parent_one = draw_parent_one(jax.random.fold_in(seeds[25], 71), 0)
    weight_one = jnp.clip(jnp.exp(math.log(0.29882812) - 1.7917595 * jax.random.uniform(seeds[6], (NF,), jnp.float32) ** steps_of(seeds[6], (NF,), ((0, 128),), -0.2, 0.2)), 0.049804688, 0.29882812).astype(jnp.bfloat16)
    coarse_src_one = draw_coarse_src_one(jax.random.fold_in(seeds[25], 71), 0)
    coarse_dst_one = touch_ends(jax.random.randint(seeds[8], (N_GX * N_GY * E1_DEV,), 0, NC1_DEV), jax.random.fold_in(seeds[8], 1), 0, NC1_DEV - 1).astype(jnp.int32)
    parent_two = draw_parent_two(jax.random.fold_in(seeds[25], 71), 0)
    weight_two = jnp.clip(jnp.exp(math.log(0.5) - 1.6133518 * jax.random.uniform(seeds[10], (NC1,), jnp.float32) ** steps_of(seeds[10], (NC1,), ((0, 128),), -0.2, 0.2)), 0.099609375, 0.5).astype(jnp.bfloat16)
    coarse_src_two = draw_coarse_src_two(jax.random.fold_in(seeds[25], 71), 0)
    coarse_dst_two = touch_ends(jax.random.randint(seeds[12], (N_GX * N_GY * E2_DEV,), 0, NC2_DEV), jax.random.fold_in(seeds[12], 1), 0, NC2_DEV - 1).astype(jnp.int32)
    fine_message_in = normal_values(seeds[13], (3 * D, D), (3 * D) ** -0.5, 0.15625)
    fine_message_out = normal_values(seeds[14], (D, D), D ** -0.5, 0.25)
    fine_message_gain = jnp.clip(1.0 + 0.15 * jax.random.normal(seeds[15], (D,), jnp.float32), 0.25, 1.75).astype(jnp.bfloat16)
    fine_update_in = normal_values(seeds[16], (2 * D, D), (2 * D) ** -0.5, 0.1875)
    fine_update_out = normal_values(seeds[17], (D, D), D ** -0.5, 0.25)
    fine_update_gain = jnp.clip(1.0 + 0.15 * jax.random.normal(seeds[18], (D,), jnp.float32), 0.25, 1.75).astype(jnp.bfloat16)
    coarse_message_in = normal_values(seeds[19], (2 * D, D), (2 * D) ** -0.5, 0.1875)
    coarse_message_out = normal_values(seeds[20], (D, D), D ** -0.5, 0.25)
    coarse_message_gain = jnp.clip(1.0 + 0.15 * jax.random.normal(seeds[21], (D,), jnp.float32), 0.25, 1.75).astype(jnp.bfloat16)
    coarse_update_in = normal_values(seeds[22], (2 * D, D), (2 * D) ** -0.5, 0.1875)
    coarse_update_out = normal_values(seeds[23], (D, D), D ** -0.5, 0.25)
    coarse_update_gain = jnp.clip(1.0 + 0.15 * jax.random.normal(seeds[24], (D,), jnp.float32), 0.25, 1.75).astype(jnp.bfloat16)
    return dict(fine_nodes=fine_nodes, edge_latent=edge_latent, boundary=boundary, fine_src=fine_src, fine_dst=fine_dst, parent_one=parent_one, weight_one=weight_one, coarse_src_one=coarse_src_one, coarse_dst_one=coarse_dst_one, parent_two=parent_two, weight_two=weight_two, coarse_src_two=coarse_src_two, coarse_dst_two=coarse_dst_two, fine_message_in=fine_message_in, fine_message_out=fine_message_out, fine_message_gain=fine_message_gain, fine_update_in=fine_update_in, fine_update_out=fine_update_out, fine_update_gain=fine_update_gain, coarse_message_in=coarse_message_in, coarse_message_out=coarse_message_out, coarse_message_gain=coarse_message_gain, coarse_update_in=coarse_update_in, coarse_update_out=coarse_update_out, coarse_update_gain=coarse_update_gain)


def normed(preact, scales):
    average = lax.optimization_barrier(jnp.mean(preact, axis=-1, keepdims=True))
    centred = preact - average
    spread = lax.optimization_barrier(jnp.mean(centred * centred, axis=-1, keepdims=True))
    return centred * lax.rsqrt(spread + 1e-05) * scales.astype(jnp.float32)

def network(inputs, project_in, project_out, scales):
    preact = jnp.dot(inputs, project_in, preferred_element_type=jnp.float32)
    hidden = jax.nn.silu(preact).astype(jnp.bfloat16)
    return normed(jnp.dot(hidden, project_out, preferred_element_type=jnp.float32), scales)

def to_global(numbers, per_device, local_count, rim_count):
    owners = jnp.arange(numbers.shape[0], dtype=jnp.int32) // per_device
    first_coord = owners // N_GY
    second_coord = owners % N_GY
    beyond = jnp.maximum(numbers - local_count, 0)
    sector = beyond // rim_count
    within = beyond % rim_count
    neighbour = (first_coord + sector // 3 - 1) % N_GX * N_GY + (second_coord + sector % 3 - 1) % N_GY
    return jnp.where(numbers < local_count, owners * local_count + numbers, neighbour * local_count + within).astype(jnp.int32)

def level_pass(states, sources, targets, node_count, message_in, message_out, message_gain, update_in, update_out, update_gain):
    inputs = jnp.concatenate([states[sources], states[targets]], axis=1)
    messages = network(inputs, message_in, message_out, message_gain).astype(jnp.bfloat16)
    incoming = jax.ops.segment_sum(messages.astype(jnp.float32), targets, num_segments=node_count).astype(jnp.bfloat16)
    update = network(jnp.concatenate([states, incoming], axis=1), update_in, update_out, update_gain)
    return (states.astype(jnp.float32) + update).astype(jnp.bfloat16)

def restrict(states, parents, weights, node_count):
    terms = weights.astype(jnp.float32)[:, None] * states.astype(jnp.float32)
    return jax.ops.segment_sum(terms, parents, num_segments=node_count).astype(jnp.bfloat16)

def reference(fine_nodes, edge_latent, boundary, fine_src, fine_dst, parent_one, weight_one, coarse_src_one, coarse_dst_one, parent_two, weight_two, coarse_src_two, coarse_dst_two, fine_message_in, fine_message_out, fine_message_gain, fine_update_in, fine_update_out, fine_update_gain, coarse_message_in, coarse_message_out, coarse_message_gain, coarse_update_in, coarse_update_out, coarse_update_gain):
    devices = N_GX * N_GY
    features = fine_nodes.shape[1]
    parent_one_global = to_global(parent_one, NF_DEV, NC1_DEV, CB1)
    coarse_src_one_global = to_global(coarse_src_one, E1_DEV, NC1_DEV, CB1)
    parent_two_global = to_global(parent_two, NC1_DEV, NC2_DEV, CB2)
    coarse_src_two_global = to_global(coarse_src_two, E2_DEV, NC2_DEV, CB2)
    device_ids = jnp.arange(devices, dtype=jnp.int32)
    flat_rows = (device_ids[:, None] * NF_DEV + boundary.reshape(devices, BND)).reshape(-1)
    chosen = fine_nodes[flat_rows].reshape(N_GX, N_GY, BND, features)
    blocks = []
    for offset_x in range(3):
        for offset_y in range(3):
            blocks.append(jnp.roll(chosen, (1 - offset_x, 1 - offset_y), axis=(0, 1)))
    beside_all = jnp.stack(blocks, axis=2).reshape(devices, 9 * BND, features)

    def one_device(packed):
        nodes, neighbours, latent, sources, targets = packed
        extended = jnp.concatenate([nodes, neighbours], axis=0)
        inputs = jnp.concatenate([extended[sources], nodes[targets], latent], axis=1)
        messages = network(inputs, fine_message_in, fine_message_out, fine_message_gain).astype(jnp.bfloat16)
        incoming = jax.ops.segment_sum(messages.astype(jnp.float32), targets, num_segments=NF_DEV).astype(jnp.bfloat16)
        update = network(jnp.concatenate([nodes, incoming], axis=1), fine_update_in, fine_update_out, fine_update_gain)
        return (nodes.astype(jnp.float32) + update).astype(jnp.bfloat16)
    fine_new = lax.map(one_device, (fine_nodes.reshape(devices, NF_DEV, features), beside_all, edge_latent.reshape(devices, E_DEV, features), fine_src.reshape(devices, E_DEV), fine_dst.reshape(devices, E_DEV)))
    fine_new = fine_new.reshape(devices * NF_DEV, features)
    level_one = restrict(fine_new, parent_one_global, weight_one, NC1)
    owner_one = jnp.arange(devices * E1_DEV, dtype=jnp.int32) // E1_DEV * NC1_DEV
    level_one_new = level_pass(level_one, coarse_src_one_global, owner_one + coarse_dst_one, NC1, coarse_message_in, coarse_message_out, coarse_message_gain, coarse_update_in, coarse_update_out, coarse_update_gain)
    level_two = restrict(level_one_new, parent_two_global, weight_two, NC2)
    owner_two = jnp.arange(devices * E2_DEV, dtype=jnp.int32) // E2_DEV * NC2_DEV
    level_two_new = level_pass(level_two, coarse_src_two_global, owner_two + coarse_dst_two, NC2, coarse_message_in, coarse_message_out, coarse_message_gain, coarse_update_in, coarse_update_out, coarse_update_gain)
    level_one_final = (level_one_new.astype(jnp.float32) + level_two_new[parent_two_global].astype(jnp.float32)).astype(jnp.bfloat16)
    return (fine_new.astype(jnp.float32) + level_one_final[parent_one_global].astype(jnp.float32)).astype(jnp.bfloat16)
```

```python
import jax
import jax.numpy as jnp
from jax import lax
from jax.experimental import pallas as pl
from jax.experimental.pallas import tpu as pltpu
from jax.sharding import PartitionSpec as P

MESH = pl.DeviceIdType.MESH
BF16 = jnp.bfloat16
F32 = jnp.float32

D = 512
NF = 1024
BND = 128
EDGES = 6144
N1, R1, E1 = 256, 64, 1536
N2, R2, E2 = 64, 32, 384
T1 = 512
T2 = 512
OFFSETS = [(k // 3 - 1, k % 3 - 1) for k in range(9) if k != 4]


def neighbours(n_gx, n_gy):
    ix, iy = lax.axis_index("gx"), lax.axis_index("gy")
    return [
        (lax.rem(ix + dx + n_gx, n_gx), lax.rem(iy + dy + n_gy, n_gy)) for dx, dy in OFFSETS
    ]


def greet(around):
    barrier = pltpu.get_barrier_semaphore()
    for who in around:
        pl.semaphore_signal(barrier, inc=1, device_id=who, device_id_type=MESH)


def all_greeted():
    pl.semaphore_wait(pltpu.get_barrier_semaphore(), 8)


def exchange(around, piece, landing, send_sem, recv_sem):
    copies = []
    for s, who in enumerate(around):
        copies.append(
            pltpu.make_async_remote_copy(
                src_ref=piece(s),
                dst_ref=landing.at[7 - s],
                send_sem=send_sem.at[s],
                recv_sem=recv_sem.at[7 - s],
                device_id=who,
                device_id_type=MESH,
            )
        )
    for copy in copies:
        copy.start()
    return copies


def finished(copies):
    for copy in copies:
        copy.wait()


def dot(a, b):
    return jnp.dot(a, b, preferred_element_type=F32)


def silu(v):
    half = 0.5 * v
    return half + half * jnp.tanh(half)


def normed(v, gain):
    centred = v - jnp.mean(v, axis=-1, keepdims=True)
    spread = jnp.mean(centred * centred, axis=-1, keepdims=True)
    return centred * lax.rsqrt(spread + 1e-05) * gain


def packed_numbers(numbers, local, rim):
    return jnp.where(numbers >= local + 5 * rim, numbers - rim, numbers)


def pick_rows(row, width, first=0):
    across = jnp.broadcast_to(row - first, (128, 128)).T
    lane = lax.broadcasted_iota(jnp.int32, (128, 128), 1)
    return jnp.concatenate(
        [
            jnp.where(across == lane + 128 * c, 1.0, 0.0).astype(BF16)
            for c in range(width // 128)
        ],
        axis=1,
    )


def pick_matrix(rows, start, count, width, first=0):
    return jnp.concatenate(
        [pick_rows(rows[:, start + j : start + j + 128], width, first) for j in range(0, count, 128)],
        axis=0,
    )


def gather_sums(rows, height):
    down = lax.broadcasted_iota(jnp.int32, (height, rows.shape[1]), 0)
    return jnp.where(down == rows, 1.0, 0.0).astype(BF16)


def halo_kernel(
    n_gx, n_gy, nodes, bnd, src, dst, latent, w_in, base, halo_out, src_out,
    target, edge_rows, halo, send_sem, recv_sem,
):
    step = pl.program_id(0)
    around = neighbours(n_gx, n_gy)

    @pl.when(step == 0)
    def _():
        greet(around)
        edge_rows[...] = dot(pick_rows(bnd[...], NF), nodes[...]).astype(BF16)
        all_greeted()
        exchange(around, lambda s: edge_rows, halo, send_sem, recv_sem)
        target[...] = dot(nodes[...], w_in[D : 2 * D]).astype(BF16)
        src_out[...] = packed_numbers(src[...], NF, BND) * 4

    base[...] = (
        dot(pick_matrix(dst[0], 0, T1, NF), target[...]) + dot(latent[...], w_in[2 * D :])
    ).astype(BF16)

    @pl.when(step == pl.num_programs(0) - 1)
    def _():
        for s, who in enumerate(around):
            pltpu.make_async_remote_copy(
                src_ref=edge_rows,
                dst_ref=halo.at[7 - s],
                send_sem=send_sem.at[s],
                recv_sem=recv_sem.at[7 - s],
                device_id=who,
                device_id_type=MESH,
            ).wait()
        for s in range(8):
            halo_out[pl.ds(s * BND, BND), :] = halo[s]


def edge_kernel(
    nodes, halo, src, dst, base, w_src, w_out, gain, up_in, up_out, up_gain, fine_new,
    table, picked, total,
):
    step = pl.program_id(0)

    def pick(first):
        for e in range(T2):
            row = pl.multiple_of(src[first + e], 4)
            picked[pl.ds(4 * e, 4), :] = table[pl.ds(row, 4), :]

    @pl.when(step == 0)
    def _():
        for c in range(0, 2 * NF, 256):
            rows = nodes[c : c + 256] if c < NF else halo[c - NF : c - NF + 256]
            value = dot(rows, w_src[...])
            for j in range(4):
                table[pl.ds(4 * c + j, 256, stride=4), :] = value[:, 128 * j : 128 * (j + 1)]
        total[...] = jnp.zeros_like(total)
        pick(0)

    source = jnp.concatenate(
        [picked[pl.ds(j, T2, stride=4), :] for j in range(4)], axis=1
    )
    hidden = silu(source + base[...].astype(F32)).astype(BF16)
    following = jnp.minimum(step + 1, pl.num_programs(0) - 1) * T2
    pick(following)
    messages = normed(dot(hidden, w_out[...]), gain[...].astype(F32)).astype(BF16)
    total[...] += dot(gather_sums(dst[0], NF), messages)

    @pl.when(step == pl.num_programs(0) - 1)
    def _():
        incoming = total[...].astype(BF16)
        states = nodes[...]
        update = silu(dot(states, up_in[:D]) + dot(incoming, up_in[D:])).astype(BF16)
        fine_new[...] = (
            states.astype(F32) + normed(dot(update, up_out[...]), up_gain[...].astype(F32))
        ).astype(BF16)


def spread_sums(states, parents, weights, local, rim):
    numbers = packed_numbers(parents, local, rim)
    down = lax.broadcasted_iota(jnp.int32, (local + 8 * rim, parents.shape[1]), 0)
    spread = jnp.where(down == numbers, weights.astype(F32), 0.0).astype(BF16)
    return dot(spread, states)


def node_update(states, incoming, up_in, up_out, up_gain):
    update = silu(dot(states, up_in[:D]) + dot(incoming, up_in[D:])).astype(BF16)
    return (
        states.astype(F32) + normed(dot(update, up_out[...]), up_gain[...].astype(F32))
    ).astype(BF16)


def coarse_kernel(
    n_gx, n_gy, fine, parent1, weight1, src1, dst1, parent2, weight2, src2, dst2,
    msg_in, msg_out, msg_gain, up_in, up_out, up_gain, out,
    sums1, land_a, level1, land_b, sums2, land_c, level2, land_d, new2, land_e, final1, land_f,
    preact, send_sem, recv_sem,
):
    around = neighbours(n_gx, n_gy)
    greet(around)

    def swap(i, piece, landing):
        return exchange(around, piece, landing, send_sem.at[i], recv_sem.at[i])

    parents = packed_numbers(parent1[...], N1, R1)
    spread = spread_sums(fine[...], parent1[...], weight1[...], N1, R1)
    sums1[...] = spread[N1:].astype(BF16)
    all_greeted()
    moving = swap(0, lambda s: sums1.at[pl.ds(s * R1, R1)], land_a)
    down_rows = gather_sums(dst1[...], N1)
    finished(moving)
    rim = spread[:R1]
    for s in range(8):
        rim = rim + land_a[s].astype(F32)
    level1[...] = jnp.concatenate([rim, spread[R1:N1]], axis=0).astype(BF16)

    moving = swap(1, lambda s: level1.at[pl.ds(0, R1)], land_b)
    own = dot(level1[...], msg_in[:D]).astype(BF16)
    mine = dot(level1[...], msg_in[D:]).astype(BF16)
    numbers = packed_numbers(src1[...], N1, R1)
    for t in range(0, E1, 512):
        preact[pl.ds(t, 512), :] = dot(pick_matrix(numbers, t, 512, N1), own) + dot(
            pick_matrix(dst1, t, 512, N1), mine
        )
    finished(moving)
    beyond = dot(land_b[...].reshape(8 * R1, D), msg_in[:D]).astype(BF16)
    incoming = jnp.zeros((N1, D), F32)
    for t in range(0, E1, 512):
        hidden = silu(
            preact[pl.ds(t, 512), :] + dot(pick_matrix(numbers, t, 512, 8 * R1, N1), beyond)
        ).astype(BF16)
        messages = normed(dot(hidden, msg_out[...]), msg_gain[...].astype(F32)).astype(BF16)
        incoming = incoming + dot(down_rows[:, t : t + 512], messages)
    new1 = node_update(level1[...], incoming.astype(BF16), up_in, up_out, up_gain)

    spread = spread_sums(new1, parent2[...], weight2[...], N2, R2)
    sums2[...] = spread[N2:].astype(BF16)
    moving = swap(2, lambda s: sums2.at[pl.ds(s * R2, R2)], land_c)
    finished(moving)
    rim = spread[:R2]
    for s in range(8):
        rim = rim + land_c[s].astype(F32)
    level2[...] = jnp.concatenate([rim, spread[R2:N2]], axis=0).astype(BF16)

    moving = swap(3, lambda s: level2.at[pl.ds(0, R2)], land_d)
    mine = dot(level2[...], msg_in[D:]).astype(BF16)
    own = dot(level2[...], msg_in[:D]).astype(BF16)
    numbers = packed_numbers(src2[...], N2, R2)
    pad = jnp.zeros((64, D), BF16)
    start = dot(pick_matrix(dst2, 0, E2, 128), jnp.concatenate([mine, pad], axis=0)) + dot(
        pick_matrix(numbers, 0, E2, 128), jnp.concatenate([own, pad], axis=0)
    )
    finished(moving)
    beyond = dot(land_d[...].reshape(8 * R2, D), msg_in[:D]).astype(BF16)
    hidden = silu(start + dot(pick_matrix(numbers, 0, E2, 8 * R2, N2), beyond)).astype(BF16)
    messages = normed(dot(hidden, msg_out[...]), msg_gain[...].astype(F32)).astype(BF16)
    incoming = dot(gather_sums(dst2[...], N2), messages).astype(BF16)
    new2[...] = node_update(level2[...], incoming, up_in, up_out, up_gain)

    moving = swap(4, lambda s: new2.at[pl.ds(0, R2)], land_e)
    numbers = packed_numbers(parent2[...], N2, R2)
    lift = new1.astype(F32) + dot(
        pick_matrix(numbers, 0, N1, 128), jnp.concatenate([new2[...], pad], axis=0)
    )
    finished(moving)
    final1[...] = (
        lift + dot(pick_matrix(numbers, 0, N1, 8 * R2, N2), land_e[...].reshape(8 * R2, D))
    ).astype(BF16)

    moving = swap(5, lambda s: final1.at[pl.ds(0, R1)], land_f)
    for t in range(0, NF, 512):
        preact[pl.ds(t, 512), :] = fine[pl.ds(t, 512), :].astype(F32) + dot(
            pick_matrix(parents, t, 512, N1), final1[...]
        )
    finished(moving)
    rims = land_f[...].reshape(8 * R1, D)
    for t in range(0, NF, 512):
        out[pl.ds(t, 512), :] = (
            preact[pl.ds(t, 512), :] + dot(pick_matrix(parents, t, 512, 8 * R1, N1), rims)
        ).astype(BF16)


def vmem():
    return pl.BlockSpec(memory_space=pltpu.VMEM)


def per_device(n_gx, n_gy, args):
    (
        fine_nodes, edge_latent, boundary, fine_src, fine_dst, parent_one, weight_one,
        coarse_src_one, coarse_dst_one, parent_two, weight_two, coarse_src_two, coarse_dst_two,
        fine_message_in, fine_message_out, fine_message_gain,
        fine_update_in, fine_update_out, fine_update_gain,
        coarse_message_in, coarse_message_out, coarse_message_gain,
        coarse_update_in, coarse_update_out, coarse_update_gain,
    ) = args

    def whole(shape):
        return pl.BlockSpec(shape, lambda i: (0,) * len(shape))

    def row(v):
        return v.reshape(1, -1)

    steps = EDGES // T1
    base, halo, src4 = pl.pallas_call(
        lambda *refs: halo_kernel(n_gx, n_gy, *refs),
        name="halo",
        grid=(steps,),
        out_shape=(
            jax.ShapeDtypeStruct((EDGES, D), BF16),
            jax.ShapeDtypeStruct((8 * BND, D), BF16),
            jax.ShapeDtypeStruct((EDGES // 128, 128), jnp.int32),
        ),
        in_specs=[
            whole((NF, D)),
            whole((1, BND)),
            whole((EDGES // 128, 128)),
            pl.BlockSpec((1, 1, T1), lambda i: (i, 0, 0)),
            pl.BlockSpec((T1, D), lambda i: (i, 0)),
            whole((3 * D, D)),
        ],
        out_specs=(
            pl.BlockSpec((T1, D), lambda i: (i, 0)),
            whole((8 * BND, D)),
            whole((EDGES // 128, 128)),
        ),
        scratch_shapes=[
            pltpu.VMEM((NF, D), BF16),
            pltpu.VMEM((BND, D), BF16),
            pltpu.VMEM((8, BND, D), BF16),
            pltpu.SemaphoreType.DMA((8,)),
            pltpu.SemaphoreType.DMA((8,)),
        ],
        compiler_params=pltpu.CompilerParams(
            collective_id=0,
            has_side_effects=True,
            vmem_limit_bytes=24 * 2**20,
            dimension_semantics=("arbitrary",),
        ),
    )(
        fine_nodes, row(boundary), fine_src.reshape(-1, 128), fine_dst.reshape(steps, 1, T1),
        edge_latent, fine_message_in,
    )

    steps = EDGES // T2
    fine_new = pl.pallas_call(
        edge_kernel,
        name="edges",
        grid=(steps,),
        out_shape=jax.ShapeDtypeStruct((NF, D), BF16),
        in_specs=[
            whole((NF, D)),
            whole((8 * BND, D)),
            pl.BlockSpec(memory_space=pltpu.SMEM),
            pl.BlockSpec((1, 1, T2), lambda i: (i, 0, 0)),
            pl.BlockSpec((T2, D), lambda i: (i, 0)),
            whole((D, D)),
            whole((D, D)),
            whole((1, D)),
            whole((2 * D, D)),
            whole((D, D)),
            whole((1, D)),
        ],
        out_specs=whole((NF, D)),
        scratch_shapes=[
            pltpu.VMEM((2 * NF * 4, 128), F32),
            pltpu.VMEM((T2 * 4, 128), F32),
            pltpu.VMEM((NF, D), F32),
        ],
        compiler_params=pltpu.CompilerParams(
            vmem_limit_bytes=40 * 2**20,
            dimension_semantics=("arbitrary",),
        ),
    )(
        fine_nodes, halo, src4.reshape(-1), fine_dst.reshape(steps, 1, T2), base,
        fine_message_in, fine_message_out, row(fine_message_gain),
        fine_update_in, fine_update_out, row(fine_update_gain),
    )

    return pl.pallas_call(
        lambda *refs: coarse_kernel(n_gx, n_gy, *refs),
        name="coarse",
        out_shape=jax.ShapeDtypeStruct((NF, D), BF16),
        in_specs=[vmem()] * 15,
        out_specs=vmem(),
        scratch_shapes=[
            pltpu.VMEM((8 * R1, D), BF16),
            pltpu.VMEM((8, R1, D), BF16),
            pltpu.VMEM((N1, D), BF16),
            pltpu.VMEM((8, R1, D), BF16),
            pltpu.VMEM((8 * R2, D), BF16),
            pltpu.VMEM((8, R2, D), BF16),
            pltpu.VMEM((N2, D), BF16),
            pltpu.VMEM((8, R2, D), BF16),
            pltpu.VMEM((N2, D), BF16),
            pltpu.VMEM((8, R2, D), BF16),
            pltpu.VMEM((N1, D), BF16),
            pltpu.VMEM((8, R1, D), BF16),
            pltpu.VMEM((E1, D), F32),
            pltpu.SemaphoreType.DMA((6, 8)),
            pltpu.SemaphoreType.DMA((6, 8)),
        ],
        compiler_params=pltpu.CompilerParams(
            collective_id=1, has_side_effects=True, vmem_limit_bytes=40 * 2**20
        ),
    )(
        fine_new, row(parent_one), row(weight_one), row(coarse_src_one), row(coarse_dst_one),
        row(parent_two), row(weight_two), row(coarse_src_two), row(coarse_dst_two),
        coarse_message_in, coarse_message_out, row(coarse_message_gain),
        coarse_update_in, coarse_update_out, row(coarse_update_gain),
    )


def solution(mesh):
    both = ("gx", "gy")
    in_specs = (P(both, None), P(both, None)) + (P(both),) * 11 + (P(),) * 12
    return jax.shard_map(
        lambda *args: per_device(mesh.shape["gx"], mesh.shape["gy"], args),
        mesh=mesh,
        in_specs=in_specs,
        out_specs=P(both, None),
        check_vma=False,
    )
```

```python
import jax
import jax.numpy as jnp
from jax import lax
from jax.experimental import pallas as pl
from jax.experimental.pallas import tpu as pltpu
from jax.sharding import PartitionSpec as P

MESH = pl.DeviceIdType.MESH
BF16 = jnp.bfloat16
F32 = jnp.float32

D = 512
NF = 1024
BND = 128
EDGES = 6144
N1, R1, E1 = 256, 64, 1536
N2, R2, E2 = 64, 32, 384
T1 = 512
T2 = 512
OFFSETS = [(k // 3 - 1, k % 3 - 1) for k in range(9) if k != 4]


def neighbours(n_gx, n_gy):
    ix, iy = lax.axis_index("gx"), lax.axis_index("gy")
    return [
        (lax.rem(ix + dx + n_gx, n_gx), lax.rem(iy + dy + n_gy, n_gy)) for dx, dy in OFFSETS
    ]


def greet(around):
    barrier = pltpu.get_barrier_semaphore()
    for who in around:
        pl.semaphore_signal(barrier, inc=1, device_id=who, device_id_type=MESH)


def all_greeted():
    pl.semaphore_wait(pltpu.get_barrier_semaphore(), 8)


def exchange(around, piece, landing, send_sem, recv_sem):
    copies = []
    for s, who in enumerate(around):
        copies.append(
            pltpu.make_async_remote_copy(
                src_ref=piece(s),
                dst_ref=landing.at[7 - s],
                send_sem=send_sem.at[s],
                recv_sem=recv_sem.at[7 - s],
                device_id=who,
                device_id_type=MESH,
            )
        )
    for copy in copies:
        copy.start()
    return copies


def finished(copies):
    for copy in copies:
        copy.wait()


def dot(a, b):
    return jnp.dot(a, b, preferred_element_type=F32)


def silu(v):
    half = 0.5 * v
    return half + half * jnp.tanh(half)


def normed(v, gain):
    centred = v - jnp.mean(v, axis=-1, keepdims=True)
    spread = jnp.mean(centred * centred, axis=-1, keepdims=True)
    return centred * lax.rsqrt(spread + 1e-05) * gain


def packed_numbers(numbers, local, rim):
    return jnp.where(numbers >= local + 5 * rim, numbers - rim, numbers)


def pick_rows(row, width, first=0):
    across = jnp.broadcast_to(row - first, (128, 128)).T
    lane = lax.broadcasted_iota(jnp.int32, (128, 128), 1)
    return jnp.concatenate(
        [
            jnp.where(across == lane + 128 * c, 1.0, 0.0).astype(BF16)
            for c in range(width // 128)
        ],
        axis=1,
    )


def pick_matrix(rows, start, count, width, first=0):
    return jnp.concatenate(
        [pick_rows(rows[:, start + j : start + j + 128], width, first) for j in range(0, count, 128)],
        axis=0,
    )


def gather_sums(rows, height):
    down = lax.broadcasted_iota(jnp.int32, (height, rows.shape[1]), 0)
    return jnp.where(down == rows, 1.0, 0.0).astype(BF16)


def spread_sums(states, parents, weights, local, rim):
    numbers = packed_numbers(parents, local, rim)
    down = lax.broadcasted_iota(jnp.int32, (local + 8 * rim, parents.shape[1]), 0)
    spread = jnp.where(down == numbers, weights, 0.0).astype(BF16)
    return dot(spread, states)


def node_update(states, incoming, up_in, up_out, up_gain):
    update = silu(dot(states, up_in[:D]) + dot(incoming, up_in[D:])).astype(BF16)
    return (
        states.astype(F32) + normed(dot(update, up_out[...]), flat_row(up_gain))
    ).astype(BF16)


def coarse_part(
    around, fine, parent1, weight1, src1, dst1, parent2, weight2, src2, dst2,
    msg_in, msg_out, msg_gain, up_in, up_out, up_gain, out,
    sums1, land_a, level1, land_b, sums2, land_c, level2, land_d, new2, land_e, final1, land_f,
    preact, send_sem, recv_sem,
):
    def swap(i, piece, landing):
        return exchange(around, piece, landing, send_sem.at[i], recv_sem.at[i])

    parents = packed_numbers(parent1[...], N1, R1)
    spread = spread_sums(fine[...], parent1[...], flat_row(weight1), N1, R1)
    sums1[...] = spread[N1:].astype(BF16)
    moving = swap(0, lambda s: sums1.at[pl.ds(s * R1, R1)], land_a)
    down_rows = gather_sums(dst1[...], N1)
    finished(moving)
    rim = spread[:R1]
    for s in range(8):
        rim = rim + land_a[s].astype(F32)
    level1[...] = jnp.concatenate([rim, spread[R1:N1]], axis=0).astype(BF16)

    moving = swap(1, lambda s: level1.at[pl.ds(0, R1)], land_b)
    own = dot(level1[...], msg_in[:D]).astype(BF16)
    mine = dot(level1[...], msg_in[D:]).astype(BF16)
    numbers = packed_numbers(src1[...], N1, R1)
    for t in range(0, E1, 512):
        preact[pl.ds(t, 512), :] = dot(pick_matrix(numbers, t, 512, N1), own) + dot(
            pick_matrix(dst1, t, 512, N1), mine
        )
    finished(moving)
    beyond = dot(land_b[...].reshape(8 * R1, D), msg_in[:D]).astype(BF16)
    incoming = jnp.zeros((N1, D), F32)
    for t in range(0, E1, 512):
        hidden = silu(
            preact[pl.ds(t, 512), :] + dot(pick_matrix(numbers, t, 512, 8 * R1, N1), beyond)
        ).astype(BF16)
        messages = normed(dot(hidden, msg_out[...]), flat_row(msg_gain)).astype(BF16)
        incoming = incoming + dot(down_rows[:, t : t + 512], messages)
    new1 = node_update(level1[...], incoming.astype(BF16), up_in, up_out, up_gain)

    spread = spread_sums(new1, parent2[...], flat_row(weight2), N2, R2)
    sums2[...] = spread[N2:].astype(BF16)
    moving = swap(2, lambda s: sums2.at[pl.ds(s * R2, R2)], land_c)
    finished(moving)
    rim = spread[:R2]
    for s in range(8):
        rim = rim + land_c[s].astype(F32)
    level2[...] = jnp.concatenate([rim, spread[R2:N2]], axis=0).astype(BF16)

    moving = swap(3, lambda s: level2.at[pl.ds(0, R2)], land_d)
    mine = dot(level2[...], msg_in[D:]).astype(BF16)
    own = dot(level2[...], msg_in[:D]).astype(BF16)
    numbers = packed_numbers(src2[...], N2, R2)
    pad = jnp.zeros((64, D), BF16)
    start = dot(pick_matrix(dst2, 0, E2, 128), jnp.concatenate([mine, pad], axis=0)) + dot(
        pick_matrix(numbers, 0, E2, 128), jnp.concatenate([own, pad], axis=0)
    )
    finished(moving)
    beyond = dot(land_d[...].reshape(8 * R2, D), msg_in[:D]).astype(BF16)
    hidden = silu(start + dot(pick_matrix(numbers, 0, E2, 8 * R2, N2), beyond)).astype(BF16)
    messages = normed(dot(hidden, msg_out[...]), flat_row(msg_gain)).astype(BF16)
    incoming = dot(gather_sums(dst2[...], N2), messages).astype(BF16)
    new2[...] = node_update(level2[...], incoming, up_in, up_out, up_gain)

    moving = swap(4, lambda s: new2.at[pl.ds(0, R2)], land_e)
    numbers = packed_numbers(parent2[...], N2, R2)
    lift = new1.astype(F32) + dot(
        pick_matrix(numbers, 0, N1, 128), jnp.concatenate([new2[...], pad], axis=0)
    )
    finished(moving)
    final1[...] = (
        lift + dot(pick_matrix(numbers, 0, N1, 8 * R2, N2), land_e[...].reshape(8 * R2, D))
    ).astype(BF16)

    moving = swap(5, lambda s: final1.at[pl.ds(0, R1)], land_f)
    for t in range(0, NF, 512):
        preact[pl.ds(t, 512), :] = fine[pl.ds(t, 512), :].astype(F32) + dot(
            pick_matrix(parents, t, 512, N1), final1[...]
        )
    finished(moving)
    rims = land_f[...].reshape(8 * R1, D)
    for t in range(0, NF, 512):
        out[pl.ds(t, 512), :] = (
            preact[pl.ds(t, 512), :] + dot(pick_matrix(parents, t, 512, 8 * R1, N1), rims)
        ).astype(BF16)


LOADS = (
    "nodes", "bnd", "w_in", "dst", "src", "w_out", "gain", "up_in", "up_out", "up_gain",
    "parent1", "weight1", "src1", "dst1", "parent2", "weight2", "src2", "dst2",
    "msg_in", "msg_out", "msg_gain", "cup_in", "cup_out", "cup_gain",
)


def flat_row(ref):
    return ref[...].astype(F32).reshape(1, -1)


def block_kernel(n_gx, n_gy, *refs):
    count = len(LOADS)
    far = dict(zip(LOADS, refs[:count]))
    latent_far, out = refs[count], refs[count + 1]
    here = dict(zip(LOADS, refs[count + 2 : 2 * count + 2]))
    (
        latent, table, picked, total, target, edge_rows, halo,
        fine, sums1, land_a, level1, land_b, sums2, land_c, level2, land_d, new2, land_e,
        final1, land_f, preact, load_sem, latent_sem, halo_send, halo_recv,
        send_sem, recv_sem,
    ) = refs[2 * count + 2 :]
    around = neighbours(n_gx, n_gy)
    greet(around)
    loads = {
        name: pltpu.make_async_copy(far[name], here[name], load_sem.at[i])
        for i, name in enumerate(LOADS)
    }

    def latent_copy(i):
        part = pl.ds(pl.multiple_of(i * T1, T1), T1)
        return pltpu.make_async_copy(latent_far.at[part], latent.at[part], latent_sem.at[i])

    for name in ("nodes", "bnd", "w_in", "dst", "src"):
        loads[name].start()
    for i in range(EDGES // T1):
        latent_copy(i).start()
    for name in LOADS[5:]:
        loads[name].start()

    nodes, dst, w_in = here["nodes"], here["dst"], here["w_in"]
    for name in ("nodes", "bnd"):
        loads[name].wait()
    edge_rows[...] = dot(pick_rows(here["bnd"][...], NF), nodes[...]).astype(BF16)
    all_greeted()
    halo_moving = exchange(around, lambda s: edge_rows, halo, halo_send, halo_recv)

    for name in ("w_in", "dst", "src"):
        loads[name].wait()
    target[...] = dot(nodes[...], w_in[D : 2 * D]).astype(BF16)

    def base_step(i, _):
        latent_copy(i).wait()
        part = pl.ds(pl.multiple_of(i * T1, T1), T1)
        latent[part, :] = (
            dot(pick_matrix(dst[i], 0, T1, NF), target[...]) + dot(latent[part, :], w_in[2 * D :])
        ).astype(BF16)
        return 0

    lax.fori_loop(0, EDGES // T1, base_step, 0)

    def fill(rows, start):
        value = dot(rows, w_in[:D])
        table[pl.ds(start, 256)] = value.reshape(256, 4, 128)

    for c in range(0, NF, 256):
        fill(nodes[pl.ds(c, 256), :], c)
    total[...] = jnp.zeros_like(total)
    for name in LOADS[5:]:
        loads[name].wait()
    finished(halo_moving)
    for s in range(0, 8, 2):
        fill(halo[pl.ds(s, 2)].reshape(2 * BND, D), NF + BND * (s + s // 4))

    def pick(first):
        for e in range(T2):
            picked[pl.ds(4 * e, 4), :] = table[here["src"][first + e]]

    pick(0)

    def edge_step(i, _):
        source = jnp.concatenate(
            [picked[pl.ds(j, T2, stride=4), :] for j in range(4)], axis=1
        )
        part = pl.ds(pl.multiple_of(i * T2, T2), T2)
        hidden = silu(source + latent[part, :].astype(F32)).astype(BF16)
        pick(jnp.minimum(i + 1, EDGES // T2 - 1) * T2)
        messages = normed(dot(hidden, here["w_out"][...]), flat_row(here["gain"])).astype(BF16)
        total[...] += dot(gather_sums(dst[i], NF), messages)
        return 0

    lax.fori_loop(0, EDGES // T2, edge_step, 0)
    fine[...] = node_update(
        nodes[...], total[...].astype(BF16), here["up_in"], here["up_out"], here["up_gain"]
    )

    coarse_part(
        around, fine, *[here[name] for name in LOADS[10:]], out,
        sums1, land_a, level1, land_b, sums2, land_c, level2, land_d, new2, land_e,
        final1, land_f, preact, send_sem, recv_sem,
    )


def per_device(n_gx, n_gy, args):
    (
        fine_nodes, edge_latent, boundary, fine_src, fine_dst, parent_one, weight_one,
        coarse_src_one, coarse_dst_one, parent_two, weight_two, coarse_src_two, coarse_dst_two,
        fine_message_in, fine_message_out, fine_message_gain,
        fine_update_in, fine_update_out, fine_update_gain,
        coarse_message_in, coarse_message_out, coarse_message_gain,
        coarse_update_in, coarse_update_out, coarse_update_gain,
    ) = args

    def row(v):
        return v.reshape(1, -1)

    given = dict(
        nodes=fine_nodes, bnd=row(boundary), w_in=fine_message_in,
        dst=fine_dst.reshape(EDGES // T1, 1, T1), src=fine_src,
        w_out=fine_message_out, gain=fine_message_gain,
        up_in=fine_update_in, up_out=fine_update_out, up_gain=fine_update_gain,
        parent1=row(parent_one), weight1=weight_one,
        src1=row(coarse_src_one), dst1=row(coarse_dst_one),
        parent2=row(parent_two), weight2=weight_two,
        src2=row(coarse_src_two), dst2=row(coarse_dst_two),
        msg_in=coarse_message_in, msg_out=coarse_message_out, msg_gain=coarse_message_gain,
        cup_in=coarse_update_in, cup_out=coarse_update_out, cup_gain=coarse_update_gain,
    )
    operands = [given[name] for name in LOADS]
    return pl.pallas_call(
        lambda *refs: block_kernel(n_gx, n_gy, *refs),
        name="block",
        out_shape=jax.ShapeDtypeStruct((NF, D), BF16),
        in_specs=[pl.BlockSpec(memory_space=pltpu.HBM)] * (len(LOADS) + 1),
        out_specs=pl.BlockSpec(memory_space=pltpu.VMEM),
        scratch_shapes=[
            (pltpu.SMEM if name == "src" else pltpu.VMEM)(v.shape, v.dtype)
            for name, v in zip(LOADS, operands)
        ]
        + [
            pltpu.VMEM((EDGES, D), BF16),
            pltpu.VMEM((NF + 9 * BND, 4, 128), F32),
            pltpu.VMEM((T2 * 4, 128), F32),
            pltpu.VMEM((NF, D), F32),
            pltpu.VMEM((NF, D), BF16),
            pltpu.VMEM((BND, D), BF16),
            pltpu.VMEM((8, BND, D), BF16),
            pltpu.VMEM((NF, D), BF16),
            pltpu.VMEM((8 * R1, D), BF16),
            pltpu.VMEM((8, R1, D), BF16),
            pltpu.VMEM((N1, D), BF16),
            pltpu.VMEM((8, R1, D), BF16),
            pltpu.VMEM((8 * R2, D), BF16),
            pltpu.VMEM((8, R2, D), BF16),
            pltpu.VMEM((N2, D), BF16),
            pltpu.VMEM((8, R2, D), BF16),
            pltpu.VMEM((N2, D), BF16),
            pltpu.VMEM((8, R2, D), BF16),
            pltpu.VMEM((N1, D), BF16),
            pltpu.VMEM((8, R1, D), BF16),
            pltpu.VMEM((E1, D), F32),
            pltpu.SemaphoreType.DMA((len(LOADS),)),
            pltpu.SemaphoreType.DMA((EDGES // T1,)),
            pltpu.SemaphoreType.DMA((8,)),
            pltpu.SemaphoreType.DMA((8,)),
            pltpu.SemaphoreType.DMA((6, 8)),
            pltpu.SemaphoreType.DMA((6, 8)),
        ],
        compiler_params=pltpu.CompilerParams(
            collective_id=0, has_side_effects=True, vmem_limit_bytes=58 * 2**20
        ),
    )(*operands, edge_latent)


def solution(mesh):
    both = ("gx", "gy")
    in_specs = (P(both, None), P(both, None)) + (P(both),) * 11 + (P(),) * 12
    return jax.shard_map(
        lambda *args: per_device(mesh.shape["gx"], mesh.shape["gy"], args),
        mesh=mesh,
        in_specs=in_specs,
        out_specs=P(both, None),
        check_vma=False,
    )
```

```python
import jax
import jax.numpy as jnp
from jax import lax
from jax.experimental import pallas as pl
from jax.experimental.pallas import tpu as pltpu
from jax.sharding import PartitionSpec as P

MESH = pl.DeviceIdType.MESH
BF16 = jnp.bfloat16
F32 = jnp.float32

D = 512
NF = 1024
BND = 128
EDGES = 6144
N1, R1, E1 = 256, 64, 1536
N2, R2, E2 = 64, 32, 384
T1 = 512
T2 = 1024
EARLY = 4
OFFSETS = [(k // 3 - 1, k % 3 - 1) for k in range(9) if k != 4]


def neighbours(n_gx, n_gy):
    ix, iy = lax.axis_index("gx"), lax.axis_index("gy")
    return [
        (lax.rem(ix + dx + n_gx, n_gx), lax.rem(iy + dy + n_gy, n_gy)) for dx, dy in OFFSETS
    ]


def greet(around):
    barrier = pltpu.get_barrier_semaphore()
    for who in around:
        pl.semaphore_signal(barrier, inc=1, device_id=who, device_id_type=MESH)


def all_greeted():
    pl.semaphore_wait(pltpu.get_barrier_semaphore(), 8)


def exchange(around, piece, landing, send_sem, recv_sem):
    copies = []
    for s, who in enumerate(around):
        copies.append(
            pltpu.make_async_remote_copy(
                src_ref=piece(s),
                dst_ref=landing.at[7 - s],
                send_sem=send_sem.at[s],
                recv_sem=recv_sem.at[7 - s],
                device_id=who,
                device_id_type=MESH,
            )
        )
    for copy in copies:
        copy.start()
    return copies


def finished(copies):
    for copy in copies:
        copy.wait()


def dot(a, b):
    return jnp.dot(a, b, preferred_element_type=F32)


def silu(v):
    half = 0.5 * v
    return half + half * jnp.tanh(half)


def normed(v, gain=None):
    centred = v - jnp.mean(v, axis=-1, keepdims=True)
    spread = jnp.mean(centred * centred, axis=-1, keepdims=True)
    scaled = centred * lax.rsqrt(spread + 1e-05)
    return scaled if gain is None else scaled * gain


def packed_numbers(numbers, local, rim):
    return jnp.where(numbers >= local + 5 * rim, numbers - rim, numbers)


def pick_rows(row, width, first=0):
    across = jnp.broadcast_to(row - first, (128, 128)).T
    lane = lax.broadcasted_iota(jnp.int32, (128, 128), 1)
    return jnp.concatenate(
        [
            jnp.where(across == lane + 128 * c, 1.0, 0.0).astype(BF16)
            for c in range(width // 128)
        ],
        axis=1,
    )


def pick_matrix(rows, start, count, width, first=0):
    return jnp.concatenate(
        [pick_rows(rows[:, start + j : start + j + 128], width, first) for j in range(0, count, 128)],
        axis=0,
    )


def gather_sums(rows, height):
    down = lax.broadcasted_iota(jnp.int32, (height, rows.shape[1]), 0)
    return jnp.where(down == rows, 1.0, 0.0).astype(BF16)


def spread_sums(states, parents, weights, local, rim):
    numbers = packed_numbers(parents, local, rim)
    down = lax.broadcasted_iota(jnp.int32, (local + 8 * rim, parents.shape[1]), 0)
    spread = jnp.where(down == numbers, weights, 0.0).astype(BF16)
    return dot(spread, states)


def node_update(states, incoming, up_in, up_out, up_gain):
    update = silu(dot(states, up_in[:D]) + dot(incoming, up_in[D:])).astype(BF16)
    return (
        states.astype(F32) + normed(dot(update, up_out[...]), flat_row(up_gain))
    ).astype(BF16)


def coarse_part(
    around, fine, parent1, weight1, src1, dst1, parent2, weight2, src2, dst2,
    msg_in, msg_out, msg_gain, up_in, up_out, up_gain, out,
    sums1, land_a, level1, land_b, sums2, land_c, level2, land_d, new2, land_e, final1, land_f,
    preact, send_sem, recv_sem,
):
    def swap(i, piece, landing):
        return exchange(around, piece, landing, send_sem.at[i], recv_sem.at[i])

    src1, dst1, src2, dst2 = (ref[...].reshape(1, -1) for ref in (src1, dst1, src2, dst2))
    parents = packed_numbers(parent1[...], N1, R1)
    spread = spread_sums(fine[...], parent1[...], flat_row(weight1), N1, R1)
    sums1[...] = spread[N1:].astype(BF16)
    moving = swap(0, lambda s: sums1.at[pl.ds(s * R1, R1)], land_a)
    down_rows = gather_sums(dst1, N1)
    finished(moving)
    rim = spread[:R1]
    for s in range(8):
        rim = rim + land_a[s].astype(F32)
    level1[...] = jnp.concatenate([rim, spread[R1:N1]], axis=0).astype(BF16)

    moving = swap(1, lambda s: level1.at[pl.ds(0, R1)], land_b)
    own = dot(level1[...], msg_in[:D]).astype(BF16)
    mine = dot(level1[...], msg_in[D:]).astype(BF16)
    numbers = packed_numbers(src1, N1, R1)
    for t in range(0, E1, 512):
        preact[pl.ds(t, 512), :] = dot(pick_matrix(numbers, t, 512, N1), own) + dot(
            pick_matrix(dst1, t, 512, N1), mine
        )
    finished(moving)
    beyond = dot(land_b[...].reshape(8 * R1, D), msg_in[:D]).astype(BF16)
    incoming = jnp.zeros((N1, D), F32)
    for t in range(0, E1, 512):
        hidden = silu(
            preact[pl.ds(t, 512), :] + dot(pick_matrix(numbers, t, 512, 8 * R1, N1), beyond)
        ).astype(BF16)
        messages = normed(dot(hidden, msg_out[...]), flat_row(msg_gain)).astype(BF16)
        incoming = incoming + dot(down_rows[:, t : t + 512], messages)
    new1 = node_update(level1[...], incoming.astype(BF16), up_in, up_out, up_gain)

    spread = spread_sums(new1, parent2[...], flat_row(weight2), N2, R2)
    sums2[...] = spread[N2:].astype(BF16)
    moving = swap(2, lambda s: sums2.at[pl.ds(s * R2, R2)], land_c)
    finished(moving)
    rim = spread[:R2]
    for s in range(8):
        rim = rim + land_c[s].astype(F32)
    level2[...] = jnp.concatenate([rim, spread[R2:N2]], axis=0).astype(BF16)

    moving = swap(3, lambda s: level2.at[pl.ds(0, R2)], land_d)
    mine = dot(level2[...], msg_in[D:]).astype(BF16)
    own = dot(level2[...], msg_in[:D]).astype(BF16)
    numbers = packed_numbers(src2, N2, R2)
    pad = jnp.zeros((64, D), BF16)
    start = dot(pick_matrix(dst2, 0, E2, 128), jnp.concatenate([mine, pad], axis=0)) + dot(
        pick_matrix(numbers, 0, E2, 128), jnp.concatenate([own, pad], axis=0)
    )
    finished(moving)
    beyond = dot(land_d[...].reshape(8 * R2, D), msg_in[:D]).astype(BF16)
    hidden = silu(start + dot(pick_matrix(numbers, 0, E2, 8 * R2, N2), beyond)).astype(BF16)
    messages = normed(dot(hidden, msg_out[...]), flat_row(msg_gain)).astype(BF16)
    incoming = dot(gather_sums(dst2, N2), messages).astype(BF16)
    new2[...] = node_update(level2[...], incoming, up_in, up_out, up_gain)

    moving = swap(4, lambda s: new2.at[pl.ds(0, R2)], land_e)
    numbers = packed_numbers(parent2[...], N2, R2)
    lift = new1.astype(F32) + dot(
        pick_matrix(numbers, 0, N1, 128), jnp.concatenate([new2[...], pad], axis=0)
    )
    finished(moving)
    final1[...] = (
        lift + dot(pick_matrix(numbers, 0, N1, 8 * R2, N2), land_e[...].reshape(8 * R2, D))
    ).astype(BF16)

    moving = swap(5, lambda s: final1.at[pl.ds(0, R1)], land_f)
    for t in range(0, NF, 512):
        preact[pl.ds(t, 512), :] = fine[pl.ds(t, 512), :].astype(F32) + dot(
            pick_matrix(parents, t, 512, N1), final1[...]
        )
    finished(moving)
    rims = land_f[...].reshape(8 * R1, D)
    for t in range(0, NF, 512):
        out[pl.ds(t, 512), :] = (
            preact[pl.ds(t, 512), :] + dot(pick_matrix(parents, t, 512, 8 * R1, N1), rims)
        ).astype(BF16)


LOADS = (
    "nodes", "bnd", "w_in", "dst", "src", "w_out", "gain", "up_in", "up_out", "up_gain",
    "parent1", "weight1", "src1", "dst1", "parent2", "weight2", "src2", "dst2",
    "msg_in", "msg_out", "msg_gain", "cup_in", "cup_out", "cup_gain",
)


def flat_row(ref):
    return ref[...].astype(F32).reshape(1, -1)


def block_kernel(n_gx, n_gy, *refs):
    count = len(LOADS)
    far = dict(zip(LOADS, refs[:count]))
    latent_far, out = refs[count], refs[count + 1]
    here = dict(zip(LOADS, refs[count + 2 : 2 * count + 2]))
    (
        latent, base, table, picked, picked_b, messages_a, messages_b, total, target, edge_rows, halo,
        fine, sums1, land_a, level1, land_b, sums2, land_c, level2, land_d, new2, land_e,
        final1, land_f, preact, load_sem, latent_sem, halo_send, halo_recv,
        send_sem, recv_sem,
    ) = refs[2 * count + 2 :]
    around = neighbours(n_gx, n_gy)
    greet(around)
    loads = {
        name: pltpu.make_async_copy(far[name], here[name], load_sem.at[i])
        for i, name in enumerate(LOADS)
    }

    def latent_copy(i):
        part = pl.ds(pl.multiple_of(i * T1, T1), T1)
        return pltpu.make_async_copy(latent_far.at[part], latent.at[part], latent_sem.at[i])

    for name in ("nodes", "bnd", "w_in", "dst", "src"):
        loads[name].start()
    for i in range(EDGES // T1):
        latent_copy(i).start()
    for name in LOADS[5:]:
        loads[name].start()

    nodes, dst, w_in = here["nodes"], here["dst"], here["w_in"]
    for name in ("nodes", "bnd"):
        loads[name].wait()
    edge_rows[...] = dot(pick_rows(here["bnd"][...], NF), nodes[...]).astype(BF16)
    for name in ("w_in", "dst", "src"):
        loads[name].wait()
    target[...] = (0.5 * dot(nodes[...], w_in[D : 2 * D])).astype(BF16)

    def base_step(i, _):
        latent_copy(i).wait()
        part = pl.ds(pl.multiple_of(i * T1, T1), T1)
        base[part, :] = dot(pick_matrix(dst[i], 0, T1, NF), target[...]) + 0.5 * dot(
            latent[part, :], w_in[2 * D :]
        )
        return 0

    lax.fori_loop(0, EARLY, base_step, 0)
    all_greeted()
    halo_moving = exchange(around, lambda s: edge_rows, halo, halo_send, halo_recv)
    lax.fori_loop(EARLY, EDGES // T1, base_step, 0)

    def fill(rows, start):
        value = 0.5 * dot(rows, w_in[:D])
        table[pl.ds(start, 256)] = value.reshape(256, 4, 128)

    for c in range(0, NF, 256):
        fill(nodes[pl.ds(c, 256), :], c)
    total[...] = jnp.zeros_like(total)
    for name in LOADS[5:]:
        loads[name].wait()
    finished(halo_moving)
    for s in range(0, 8, 2):
        fill(halo[pl.ds(s, 2)].reshape(2 * BND, D), NF + BND * (s + s // 4))

    quarter = T2 // 4

    def pick(rows, i, t):
        for e in range(quarter * t, quarter * (t + 1)):
            rows[pl.ds(4 * e, 4), :] = table[here["src"][i * T2 + e]]

    def edge_sums(messages, i, t):
        numbers = jnp.concatenate(
            [dst[i * (T2 // T1) + u] for u in range(T2 // T1)], axis=1
        ) - NF // 4 * t
        part = pl.ds(NF // 4 * t, NF // 4)
        total[part, :] += dot(gather_sums(numbers, NF // 4), messages[...])

    def edge_group(i, rows, messages, next_rows, last_messages):
        last = jnp.maximum(i - 1, 0)
        for t in range(4):
            part = pl.ds(pl.multiple_of(i * T2 + quarter * t, quarter), quarter)
            half = base[part, :] + jnp.concatenate(
                [rows[pl.ds(4 * quarter * t + j, quarter, stride=4), :] for j in range(4)],
                axis=1,
            )
            hidden = (half + half * jnp.tanh(half)).astype(BF16)
            pick(next_rows, jnp.minimum(i + 1, EDGES // T2 - 1), t)
            messages[pl.ds(quarter * t, quarter), :] = normed(
                dot(hidden, here["w_out"][...])
            ).astype(BF16)
            edge_sums(last_messages, last, t)

    def edge_step(k, _):
        edge_group(2 * k, picked, messages_a, picked_b, messages_b)
        edge_group(2 * k + 1, picked_b, messages_b, picked, messages_a)
        return 0

    messages_b[...] = jnp.zeros_like(messages_b)
    for t in range(4):
        pick(picked, 0, t)
    lax.fori_loop(0, EDGES // T2 // 2, edge_step, 0)
    for t in range(4):
        edge_sums(messages_b, EDGES // T2 - 1, t)
    total[...] = total[...] * flat_row(here["gain"])
    fine[...] = node_update(
        nodes[...], total[...].astype(BF16), here["up_in"], here["up_out"], here["up_gain"]
    )

    coarse_part(
        around, fine, *[here[name] for name in LOADS[10:]], out,
        sums1, land_a, level1, land_b, sums2, land_c, level2, land_d, new2, land_e,
        final1, land_f, preact, send_sem, recv_sem,
    )


def per_device(n_gx, n_gy, args):
    (
        fine_nodes, edge_latent, boundary, fine_src, fine_dst, parent_one, weight_one,
        coarse_src_one, coarse_dst_one, parent_two, weight_two, coarse_src_two, coarse_dst_two,
        fine_message_in, fine_message_out, fine_message_gain,
        fine_update_in, fine_update_out, fine_update_gain,
        coarse_message_in, coarse_message_out, coarse_message_gain,
        coarse_update_in, coarse_update_out, coarse_update_gain,
    ) = args

    def row(v):
        return v.reshape(1, -1)

    given = dict(
        nodes=fine_nodes, bnd=row(boundary), w_in=fine_message_in,
        dst=fine_dst.reshape(EDGES // T1, 1, T1), src=fine_src,
        w_out=fine_message_out, gain=fine_message_gain,
        up_in=fine_update_in, up_out=fine_update_out, up_gain=fine_update_gain,
        parent1=row(parent_one), weight1=weight_one,
        src1=coarse_src_one, dst1=coarse_dst_one,
        parent2=row(parent_two), weight2=weight_two,
        src2=coarse_src_two, dst2=coarse_dst_two,
        msg_in=coarse_message_in, msg_out=coarse_message_out, msg_gain=coarse_message_gain,
        cup_in=coarse_update_in, cup_out=coarse_update_out, cup_gain=coarse_update_gain,
    )
    operands = [given[name] for name in LOADS]
    return pl.pallas_call(
        lambda *refs: block_kernel(n_gx, n_gy, *refs),
        name="block",
        out_shape=jax.ShapeDtypeStruct((NF, D), BF16),
        in_specs=[pl.BlockSpec(memory_space=pltpu.HBM)] * (len(LOADS) + 1),
        out_specs=pl.BlockSpec(memory_space=pltpu.VMEM),
        scratch_shapes=[
            (pltpu.SMEM if name == "src" else pltpu.VMEM)(v.shape, v.dtype)
            for name, v in zip(LOADS, operands)
        ]
        + [
            pltpu.VMEM((EDGES, D), BF16),
            pltpu.VMEM((EDGES, D), F32),
            pltpu.VMEM((NF + 9 * BND, 4, 128), F32),
            pltpu.VMEM((T2 * 4, 128), F32),
            pltpu.VMEM((T2 * 4, 128), F32),
            pltpu.VMEM((T2, D), BF16),
            pltpu.VMEM((T2, D), BF16),
            pltpu.VMEM((NF, D), F32),
            pltpu.VMEM((NF, D), BF16),
            pltpu.VMEM((BND, D), BF16),
            pltpu.VMEM((8, BND, D), BF16),
            pltpu.VMEM((NF, D), BF16),
            pltpu.VMEM((8 * R1, D), BF16),
            pltpu.VMEM((8, R1, D), BF16),
            pltpu.VMEM((N1, D), BF16),
            pltpu.VMEM((8, R1, D), BF16),
            pltpu.VMEM((8 * R2, D), BF16),
            pltpu.VMEM((8, R2, D), BF16),
            pltpu.VMEM((N2, D), BF16),
            pltpu.VMEM((8, R2, D), BF16),
            pltpu.VMEM((N2, D), BF16),
            pltpu.VMEM((8, R2, D), BF16),
            pltpu.VMEM((N1, D), BF16),
            pltpu.VMEM((8, R1, D), BF16),
            pltpu.VMEM((E1, D), F32),
            pltpu.SemaphoreType.DMA((len(LOADS),)),
            pltpu.SemaphoreType.DMA((EDGES // T1,)),
            pltpu.SemaphoreType.DMA((8,)),
            pltpu.SemaphoreType.DMA((8,)),
            pltpu.SemaphoreType.DMA((6, 8)),
            pltpu.SemaphoreType.DMA((6, 8)),
        ],
        compiler_params=pltpu.CompilerParams(
            collective_id=0, has_side_effects=True, vmem_limit_bytes=58 * 2**20
        ),
    )(*operands, edge_latent)


def solution(mesh):
    both = ("gx", "gy")
    in_specs = (P(both, None), P(both, None)) + (P(both),) * 11 + (P(),) * 12
    return jax.shard_map(
        lambda *args: per_device(mesh.shape["gx"], mesh.shape["gy"], args),
        mesh=mesh,
        in_specs=in_specs,
        out_specs=P(both, None),
        check_vma=False,
    )
```

```python
import jax
import jax.numpy as jnp
from jax import lax
from jax.experimental import pallas as pl
from jax.experimental.pallas import tpu as pltpu
from jax.sharding import PartitionSpec as P

MESH = pl.DeviceIdType.MESH
BF16 = jnp.bfloat16
F32 = jnp.float32

D = 512
NF = 1024
BND = 128
EDGES = 6144
N1, R1, E1 = 256, 64, 1536
N2, R2, E2 = 64, 32, 384
T1 = 512
T2 = 1024
EARLY = 4
PIECES = 2
OFFSETS = [(k // 3 - 1, k % 3 - 1) for k in range(9) if k != 4]


def neighbours(n_gx, n_gy):
    ix, iy = lax.axis_index("gx"), lax.axis_index("gy")
    return [
        (lax.rem(ix + dx + n_gx, n_gx), lax.rem(iy + dy + n_gy, n_gy)) for dx, dy in OFFSETS
    ]


def greet(around):
    barrier = pltpu.get_barrier_semaphore()
    for who in around:
        pl.semaphore_signal(barrier, inc=1, device_id=who, device_id_type=MESH)


def all_greeted():
    pl.semaphore_wait(pltpu.get_barrier_semaphore(), 8)


def exchange(around, piece, landing, send_sem, recv_sem):
    copies = []
    for s, who in enumerate(around):
        copies.append(
            pltpu.make_async_remote_copy(
                src_ref=piece(s),
                dst_ref=landing.at[7 - s],
                send_sem=send_sem.at[s],
                recv_sem=recv_sem.at[7 - s],
                device_id=who,
                device_id_type=MESH,
            )
        )
    for copy in copies:
        copy.start()
    return copies


def finished(copies):
    for copy in copies:
        copy.wait()


def dot(a, b):
    return jnp.dot(a, b, preferred_element_type=F32)


def silu(v):
    half = 0.5 * v
    return half + half * jnp.tanh(half)


def normed(v, gain=None):
    centred = v - jnp.mean(v, axis=-1, keepdims=True)
    spread = jnp.mean(centred * centred, axis=-1, keepdims=True)
    scaled = centred * lax.rsqrt(spread + 1e-05)
    return scaled if gain is None else scaled * gain


def packed_numbers(numbers, local, rim):
    return jnp.where(numbers >= local + 5 * rim, numbers - rim, numbers)


def pick_rows(row, width, first=0):
    across = jnp.broadcast_to(row - first, (128, 128)).T
    lane = lax.broadcasted_iota(jnp.int32, (128, 128), 1)
    return jnp.concatenate(
        [
            jnp.where(across == lane + 128 * c, 1.0, 0.0).astype(BF16)
            for c in range(width // 128)
        ],
        axis=1,
    )


def pick_matrix(rows, start, count, width, first=0):
    return jnp.concatenate(
        [pick_rows(rows[:, start + j : start + j + 128], width, first) for j in range(0, count, 128)],
        axis=0,
    )


def gather_sums(rows, height):
    down = lax.broadcasted_iota(jnp.int32, (height, rows.shape[1]), 0)
    return jnp.where(down == rows, 1.0, 0.0).astype(BF16)


def spread_sums(states, numbers, weights, height):
    down = lax.broadcasted_iota(jnp.int32, (height, numbers.shape[1]), 0)
    spread = jnp.where(down == numbers, weights, 0.0).astype(BF16)
    return dot(spread, states)


def node_update(states, first, incoming, up_in, up_out, up_gain):
    update = silu(first + dot(incoming, up_in[D:])).astype(BF16)
    return (
        states.astype(F32) + normed(dot(update, up_out[...]), flat_row(up_gain))
    ).astype(BF16)


def coarse_part(
    around, fine, parent1, weight1, src1, dst1, parent2, weight2, src2, dst2,
    msg_in, msg_out, msg_gain, up_in, up_out, up_gain, out,
    sums1, land_a, level1, land_b, sums2, land_c, level2, land_d, new2, land_e, final1, land_f,
    preact, send_sem, recv_sem, piece_send, piece_recv,
):
    def swap(i, piece, landing):
        return exchange(around, piece, landing, send_sem.at[i], recv_sem.at[i])

    src1, dst1, src2, dst2 = (ref[...].reshape(1, -1) for ref in (src1, dst1, src2, dst2))
    parents = packed_numbers(parent1[...], N1, R1)
    weights = flat_row(weight1)
    sums1[...] = spread_sums(fine[...], parents - N1, weights, 8 * R1).astype(BF16)
    part = R1 // PIECES

    def piecewise(i, piece, landing):
        def start(h):
            copies = [
                pltpu.make_async_remote_copy(
                    src_ref=piece(s, h),
                    dst_ref=landing.at[7 - s, pl.ds(part * h, part)],
                    send_sem=piece_send.at[i, h, s],
                    recv_sem=piece_recv.at[i, h, 7 - s],
                    device_id=who,
                    device_id_type=MESH,
                )
                for s, who in enumerate(around)
            ]
            for copy in copies:
                copy.start()
            return copies

        return start

    send_sums = piecewise(0, lambda s, h: sums1.at[pl.ds(s * R1 + part * h, part)], land_a)
    send_rim = piecewise(1, lambda s, h: level1.at[pl.ds(part * h, part)], land_b)
    arriving = [send_sums(h) for h in range(PIECES)]
    spread = spread_sums(fine[...], parents, weights, N1)
    level1[pl.ds(R1, N1 - R1), :] = spread[R1:].astype(BF16)
    down_rows = gather_sums(dst1, N1)
    moving = []
    for h in range(PIECES):
        finished(arriving[h])
        rim = spread[part * h : part * (h + 1)]
        for s in range(8):
            rim = rim + land_a[s, pl.ds(part * h, part)].astype(F32)
        level1[pl.ds(part * h, part), :] = rim.astype(BF16)
        moving = moving + send_rim(h)
    own = dot(level1[...], msg_in[:D]).astype(BF16)
    mine = dot(level1[...], msg_in[D:]).astype(BF16)
    numbers = packed_numbers(src1, N1, R1)
    for t in range(0, E1, 512):
        preact[pl.ds(t, 512), :] = dot(pick_matrix(numbers, t, 512, N1), own) + dot(
            pick_matrix(dst1, t, 512, N1), mine
        )
    first = dot(level1[...], up_in[:D])
    finished(moving)
    beyond = dot(land_b[...].reshape(8 * R1, D), msg_in[:D]).astype(BF16)
    incoming = jnp.zeros((N1, D), F32)
    for t in range(0, E1, 512):
        hidden = silu(
            preact[pl.ds(t, 512), :] + dot(pick_matrix(numbers, t, 512, 8 * R1, N1), beyond)
        ).astype(BF16)
        messages = normed(dot(hidden, msg_out[...]), flat_row(msg_gain)).astype(BF16)
        incoming = incoming + dot(down_rows[:, t : t + 512], messages)
    new1 = node_update(level1[...], first, incoming.astype(BF16), up_in, up_out, up_gain)

    parents2 = packed_numbers(parent2[...], N2, R2)
    weights = flat_row(weight2)
    sums2[...] = spread_sums(new1, parents2 - N2, weights, 8 * R2).astype(BF16)
    moving = swap(2, lambda s: sums2.at[pl.ds(s * R2, R2)], land_c)
    spread = spread_sums(new1, parents2, weights, N2)
    finished(moving)
    rim = spread[:R2]
    for s in range(8):
        rim = rim + land_c[s].astype(F32)
    level2[...] = jnp.concatenate([rim, spread[R2:N2]], axis=0).astype(BF16)

    moving = swap(3, lambda s: level2.at[pl.ds(0, R2)], land_d)
    mine = dot(level2[...], msg_in[D:]).astype(BF16)
    own = dot(level2[...], msg_in[:D]).astype(BF16)
    numbers = packed_numbers(src2, N2, R2)
    pad = jnp.zeros((64, D), BF16)
    start = dot(pick_matrix(dst2, 0, E2, 128), jnp.concatenate([mine, pad], axis=0)) + dot(
        pick_matrix(numbers, 0, E2, 128), jnp.concatenate([own, pad], axis=0)
    )
    first = dot(level2[...], up_in[:D])
    finished(moving)
    beyond = dot(land_d[...].reshape(8 * R2, D), msg_in[:D]).astype(BF16)
    hidden = silu(start + dot(pick_matrix(numbers, 0, E2, 8 * R2, N2), beyond)).astype(BF16)
    messages = normed(dot(hidden, msg_out[...]), flat_row(msg_gain)).astype(BF16)
    incoming = dot(gather_sums(dst2, N2), messages).astype(BF16)
    new2[...] = node_update(level2[...], first, incoming, up_in, up_out, up_gain)

    moving = swap(4, lambda s: new2.at[pl.ds(0, R2)], land_e)
    numbers = packed_numbers(parent2[...], N2, R2)
    lift = new1.astype(F32) + dot(
        pick_matrix(numbers, 0, N1, 128), jnp.concatenate([new2[...], pad], axis=0)
    )
    finished(moving)
    final1[...] = (
        lift + dot(pick_matrix(numbers, 0, N1, 8 * R2, N2), land_e[...].reshape(8 * R2, D))
    ).astype(BF16)

    moving = swap(5, lambda s: final1.at[pl.ds(0, R1)], land_f)
    for t in range(0, NF, 512):
        preact[pl.ds(t, 512), :] = fine[pl.ds(t, 512), :].astype(F32) + dot(
            pick_matrix(parents, t, 512, N1), final1[...]
        )
    finished(moving)
    rims = land_f[...].reshape(8 * R1, D)
    for t in range(0, NF, 512):
        out[pl.ds(t, 512), :] = (
            preact[pl.ds(t, 512), :] + dot(pick_matrix(parents, t, 512, 8 * R1, N1), rims)
        ).astype(BF16)


LOADS = (
    "nodes", "bnd", "w_in", "dst", "src", "w_out", "gain", "up_in", "up_out", "up_gain",
    "parent1", "weight1", "src1", "dst1", "parent2", "weight2", "src2", "dst2",
    "msg_in", "msg_out", "msg_gain", "cup_in", "cup_out", "cup_gain",
)


def flat_row(ref):
    return ref[...].astype(F32).reshape(1, -1)


def block_kernel(n_gx, n_gy, *refs):
    count = len(LOADS)
    far = dict(zip(LOADS, refs[:count]))
    latent_far, out = refs[count], refs[count + 1]
    here = dict(zip(LOADS, refs[count + 2 : 2 * count + 2]))
    (
        latent, base, first, table, picked, messages_a, messages_b, total, target, edge_rows, halo,
        fine, sums1, land_a, level1, land_b, sums2, land_c, level2, land_d, new2, land_e,
        final1, land_f, preact, load_sem, latent_sem, halo_send, halo_recv,
        send_sem, recv_sem, piece_send, piece_recv,
    ) = refs[2 * count + 2 :]
    around = neighbours(n_gx, n_gy)
    greet(around)
    loads = {
        name: pltpu.make_async_copy(far[name], here[name], load_sem.at[i])
        for i, name in enumerate(LOADS)
    }

    def latent_copy(i):
        part = pl.ds(pl.multiple_of(i * T1, T1), T1)
        return pltpu.make_async_copy(latent_far.at[part], latent.at[part], latent_sem.at[i])

    for name in ("nodes", "bnd", "w_in", "dst", "src"):
        loads[name].start()
    for i in range(EDGES // T1):
        latent_copy(i).start()
    for name in LOADS[5:]:
        loads[name].start()

    nodes, dst, w_in = here["nodes"], here["dst"], here["w_in"]
    for name in ("nodes", "bnd"):
        loads[name].wait()
    edge_rows[...] = dot(pick_rows(here["bnd"][...], NF), nodes[...]).astype(BF16)
    for name in ("w_in", "dst", "src"):
        loads[name].wait()
    target[...] = (0.5 * dot(nodes[...], w_in[D : 2 * D])).astype(BF16)

    def base_step(i, _):
        latent_copy(i).wait()
        part = pl.ds(pl.multiple_of(i * T1, T1), T1)
        base[part, :] = dot(pick_matrix(dst[i], 0, T1, NF), target[...]) + 0.5 * dot(
            latent[part, :], w_in[2 * D :]
        )
        return 0

    lax.fori_loop(0, EARLY, base_step, 0)
    all_greeted()
    halo_moving = exchange(around, lambda s: edge_rows, halo, halo_send, halo_recv)
    lax.fori_loop(EARLY, EDGES // T1, base_step, 0)

    def fill(rows, start):
        value = 0.5 * dot(rows, w_in[:D])
        table[pl.ds(start, 256)] = value.reshape(256, 4, 128)

    for c in range(0, NF, 256):
        fill(nodes[pl.ds(c, 256), :], c)
    total[...] = jnp.zeros_like(total)
    for name in LOADS[5:]:
        loads[name].wait()
    first[...] = dot(nodes[...], here["up_in"][:D])
    finished(halo_moving)
    for s in range(0, 8, 2):
        fill(halo[pl.ds(s, 2)].reshape(2 * BND, D), NF + BND * (s + s // 4))

    quarter = T2 // 4

    def pick(rows, i, t):
        for e in range(quarter):
            rows[pl.ds(4 * e, 4), :] = table[here["src"][i * T2 + quarter * t + e]]

    def edge_sums(messages, i, t):
        numbers = jnp.concatenate(
            [dst[i * (T2 // T1) + u] for u in range(T2 // T1)], axis=1
        ) - NF // 4 * t
        part = pl.ds(NF // 4 * t, NF // 4)
        total[part, :] += dot(gather_sums(numbers, NF // 4), messages[...])

    def edge_group(i, messages, last_messages):
        last = jnp.maximum(i - 1, 0)
        following = jnp.minimum(i + 1, EDGES // T2 - 1)
        for t in range(4):
            part = pl.ds(pl.multiple_of(i * T2 + quarter * t, quarter), quarter)
            half = base[part, :] + jnp.concatenate(
                [picked[t % 2, pl.ds(j, quarter, stride=4), :] for j in range(4)],
                axis=1,
            )
            hidden = (half + half * jnp.tanh(half)).astype(BF16)
            pick(picked.at[(t + 1) % 2], i if t < 3 else following, (t + 1) % 4)
            messages[pl.ds(quarter * t, quarter), :] = normed(
                dot(hidden, here["w_out"][...])
            ).astype(BF16)
            edge_sums(last_messages, last, t)

    def edge_step(k, _):
        edge_group(2 * k, messages_a, messages_b)
        edge_group(2 * k + 1, messages_b, messages_a)
        return 0

    messages_b[...] = jnp.zeros_like(messages_b)
    pick(picked.at[0], 0, 0)
    lax.fori_loop(0, EDGES // T2 // 2, edge_step, 0)
    for t in range(4):
        edge_sums(messages_b, EDGES // T2 - 1, t)
    total[...] = total[...] * flat_row(here["gain"])
    fine[...] = node_update(
        nodes[...], first[...], total[...].astype(BF16), here["up_in"], here["up_out"], here["up_gain"]
    )

    coarse_part(
        around, fine, *[here[name] for name in LOADS[10:]], out,
        sums1, land_a, level1, land_b, sums2, land_c, level2, land_d, new2, land_e,
        final1, land_f, preact, send_sem, recv_sem, piece_send, piece_recv,
    )


def per_device(n_gx, n_gy, args):
    (
        fine_nodes, edge_latent, boundary, fine_src, fine_dst, parent_one, weight_one,
        coarse_src_one, coarse_dst_one, parent_two, weight_two, coarse_src_two, coarse_dst_two,
        fine_message_in, fine_message_out, fine_message_gain,
        fine_update_in, fine_update_out, fine_update_gain,
        coarse_message_in, coarse_message_out, coarse_message_gain,
        coarse_update_in, coarse_update_out, coarse_update_gain,
    ) = args

    def row(v):
        return v.reshape(1, -1)

    given = dict(
        nodes=fine_nodes, bnd=row(boundary), w_in=fine_message_in,
        dst=fine_dst.reshape(EDGES // T1, 1, T1), src=fine_src,
        w_out=fine_message_out, gain=fine_message_gain,
        up_in=fine_update_in, up_out=fine_update_out, up_gain=fine_update_gain,
        parent1=row(parent_one), weight1=weight_one,
        src1=coarse_src_one, dst1=coarse_dst_one,
        parent2=row(parent_two), weight2=weight_two,
        src2=coarse_src_two, dst2=coarse_dst_two,
        msg_in=coarse_message_in, msg_out=coarse_message_out, msg_gain=coarse_message_gain,
        cup_in=coarse_update_in, cup_out=coarse_update_out, cup_gain=coarse_update_gain,
    )
    operands = [given[name] for name in LOADS]
    return pl.pallas_call(
        lambda *refs: block_kernel(n_gx, n_gy, *refs),
        name="block",
        out_shape=jax.ShapeDtypeStruct((NF, D), BF16),
        in_specs=[pl.BlockSpec(memory_space=pltpu.HBM)] * (len(LOADS) + 1),
        out_specs=pl.BlockSpec(memory_space=pltpu.VMEM),
        scratch_shapes=[
            (pltpu.SMEM if name == "src" else pltpu.VMEM)(v.shape, v.dtype)
            for name, v in zip(LOADS, operands)
        ]
        + [
            pltpu.VMEM((EDGES, D), BF16),
            pltpu.VMEM((EDGES, D), F32),
            pltpu.VMEM((NF, D), F32),
            pltpu.VMEM((NF + 9 * BND, 4, 128), F32),
            pltpu.VMEM((2, T2, 128), F32),
            pltpu.VMEM((T2, D), BF16),
            pltpu.VMEM((T2, D), BF16),
            pltpu.VMEM((NF, D), F32),
            pltpu.VMEM((NF, D), BF16),
            pltpu.VMEM((BND, D), BF16),
            pltpu.VMEM((8, BND, D), BF16),
            pltpu.VMEM((NF, D), BF16),
            pltpu.VMEM((8 * R1, D), BF16),
            pltpu.VMEM((8, R1, D), BF16),
            pltpu.VMEM((N1, D), BF16),
            pltpu.VMEM((8, R1, D), BF16),
            pltpu.VMEM((8 * R2, D), BF16),
            pltpu.VMEM((8, R2, D), BF16),
            pltpu.VMEM((N2, D), BF16),
            pltpu.VMEM((8, R2, D), BF16),
            pltpu.VMEM((N2, D), BF16),
            pltpu.VMEM((8, R2, D), BF16),
            pltpu.VMEM((N1, D), BF16),
            pltpu.VMEM((8, R1, D), BF16),
            pltpu.VMEM((E1, D), F32),
            pltpu.SemaphoreType.DMA((len(LOADS),)),
            pltpu.SemaphoreType.DMA((EDGES // T1,)),
            pltpu.SemaphoreType.DMA((8,)),
            pltpu.SemaphoreType.DMA((8,)),
            pltpu.SemaphoreType.DMA((6, 8)),
            pltpu.SemaphoreType.DMA((6, 8)),
            pltpu.SemaphoreType.DMA((2, PIECES, 8)),
            pltpu.SemaphoreType.DMA((2, PIECES, 8)),
        ],
        compiler_params=pltpu.CompilerParams(
            collective_id=0, has_side_effects=True, vmem_limit_bytes=58 * 2**20
        ),
    )(*operands, edge_latent)


def solution(mesh):
    both = ("gx", "gy")
    in_specs = (P(both, None), P(both, None)) + (P(both),) * 11 + (P(),) * 12
    return jax.shard_map(
        lambda *args: per_device(mesh.shape["gx"], mesh.shape["gy"], args),
        mesh=mesh,
        in_specs=in_specs,
        out_specs=P(both, None),
        check_vma=False,
    )
```

```python
import jax
import jax.numpy as jnp
from jax import lax
from jax.experimental import pallas as pl
from jax.experimental.pallas import tpu as pltpu
from jax.sharding import PartitionSpec as P

MESH = pl.DeviceIdType.MESH
BF16 = jnp.bfloat16
F32 = jnp.float32

D = 512
NF = 1024
BND = 128
EDGES = 6144
N1, R1, E1 = 256, 64, 1536
N2, R2, E2 = 64, 32, 384
T1 = 512
T2 = 1024
EARLY = 4
PIECES = 2
OFFSETS = [(k // 3 - 1, k % 3 - 1) for k in range(9) if k != 4]


def neighbours(n_gx, n_gy):
    ix, iy = lax.axis_index("gx"), lax.axis_index("gy")
    return [
        (lax.rem(ix + dx + n_gx, n_gx), lax.rem(iy + dy + n_gy, n_gy)) for dx, dy in OFFSETS
    ]


def greet(around):
    barrier = pltpu.get_barrier_semaphore()
    for who in around:
        pl.semaphore_signal(barrier, inc=1, device_id=who, device_id_type=MESH)


def all_greeted():
    pl.semaphore_wait(pltpu.get_barrier_semaphore(), 8)


def exchange(around, piece, landing, send_sem, recv_sem):
    copies = []
    for s, who in enumerate(around):
        copies.append(
            pltpu.make_async_remote_copy(
                src_ref=piece(s),
                dst_ref=landing.at[7 - s],
                send_sem=send_sem.at[s],
                recv_sem=recv_sem.at[7 - s],
                device_id=who,
                device_id_type=MESH,
            )
        )
    for copy in copies:
        copy.start()
    return copies


def finished(copies):
    for copy in copies:
        copy.wait()


def dot(a, b):
    return jnp.dot(a, b, preferred_element_type=F32)


def silu(v):
    half = 0.5 * v
    return half + half * jnp.tanh(half)


def normed(v, gain=None):
    centred = v - jnp.mean(v, axis=-1, keepdims=True)
    spread = jnp.mean(centred * centred, axis=-1, keepdims=True)
    scaled = centred * lax.rsqrt(spread + 1e-05)
    return scaled if gain is None else scaled * gain


def packed_numbers(numbers, local, rim):
    return jnp.where(numbers >= local + 5 * rim, numbers - rim, numbers)


def pick_rows(row, width, first=0):
    across = jnp.broadcast_to(row - first, (128, 128)).T
    lane = lax.broadcasted_iota(jnp.int32, (128, 128), 1)
    return jnp.concatenate(
        [
            jnp.where(across == lane + 128 * c, 1.0, 0.0).astype(BF16)
            for c in range(width // 128)
        ],
        axis=1,
    )


def pick_matrix(rows, start, count, width, first=0):
    return jnp.concatenate(
        [pick_rows(rows[:, start + j : start + j + 128], width, first) for j in range(0, count, 128)],
        axis=0,
    )


def gather_sums(rows, height):
    down = lax.broadcasted_iota(jnp.int32, (height, rows.shape[1]), 0)
    return jnp.where(down == rows, 1.0, 0.0).astype(BF16)


def spread_sums(states, numbers, weights, height):
    down = lax.broadcasted_iota(jnp.int32, (height, numbers.shape[1]), 0)
    spread = jnp.where(down == numbers, weights, 0.0).astype(BF16)
    return dot(spread, states)


def node_update(states, first, incoming, up_in, up_out, up_gain):
    update = silu(first + dot(incoming, up_in[D:])).astype(BF16)
    return (
        states.astype(F32) + normed(dot(update, up_out[...]), flat_row(up_gain))
    ).astype(BF16)


def coarse_part(
    around, fine, parent1, weight1, src1, dst1, parent2, weight2, src2, dst2,
    msg_in, msg_out, msg_gain, up_in, up_out, up_gain, out,
    sums1, land_a, level1, land_b, sums2, land_c, level2, land_d, new2, land_e, final1, land_f,
    preact, send_sem, recv_sem, piece_send, piece_recv,
):
    def swap(i, piece, landing):
        return exchange(around, piece, landing, send_sem.at[i], recv_sem.at[i])

    src1, dst1, src2, dst2 = (ref[...].reshape(1, -1) for ref in (src1, dst1, src2, dst2))
    parents = packed_numbers(parent1[...], N1, R1)
    weights = flat_row(weight1)
    sums1[...] = spread_sums(fine[...], parents - N1, weights, 8 * R1).astype(BF16)
    part = R1 // PIECES

    def piecewise(i, part, piece, landing):
        def start(h):
            copies = [
                pltpu.make_async_remote_copy(
                    src_ref=piece(s, h),
                    dst_ref=landing.at[7 - s, pl.ds(part * h, part)],
                    send_sem=piece_send.at[i, h, s],
                    recv_sem=piece_recv.at[i, h, 7 - s],
                    device_id=who,
                    device_id_type=MESH,
                )
                for s, who in enumerate(around)
            ]
            for copy in copies:
                copy.start()
            return copies

        return start

    send_sums = piecewise(0, part, lambda s, h: sums1.at[pl.ds(s * R1 + part * h, part)], land_a)
    send_rim = piecewise(1, part, lambda s, h: level1.at[pl.ds(part * h, part)], land_b)
    arriving = [send_sums(h) for h in range(PIECES)]
    spread = spread_sums(fine[...], parents, weights, N1)
    level1[pl.ds(R1, N1 - R1), :] = spread[R1:].astype(BF16)
    down_rows = gather_sums(dst1, N1)
    moving = []
    for h in range(PIECES):
        finished(arriving[h])
        rim = spread[part * h : part * (h + 1)]
        for s in range(8):
            rim = rim + land_a[s, pl.ds(part * h, part)].astype(F32)
        level1[pl.ds(part * h, part), :] = rim.astype(BF16)
        moving = moving + send_rim(h)
    own = dot(level1[...], msg_in[:D]).astype(BF16)
    mine = dot(level1[...], msg_in[D:]).astype(BF16)
    numbers = packed_numbers(src1, N1, R1)
    for t in range(0, E1, 512):
        preact[pl.ds(t, 512), :] = dot(pick_matrix(numbers, t, 512, N1), own) + dot(
            pick_matrix(dst1, t, 512, N1), mine
        )
    first = dot(level1[...], up_in[:D])
    finished(moving)
    beyond = dot(land_b[...].reshape(8 * R1, D), msg_in[:D]).astype(BF16)
    incoming = jnp.zeros((N1, D), F32)
    for t in range(0, E1, 512):
        hidden = silu(
            preact[pl.ds(t, 512), :] + dot(pick_matrix(numbers, t, 512, 8 * R1, N1), beyond)
        ).astype(BF16)
        messages = normed(dot(hidden, msg_out[...]), flat_row(msg_gain)).astype(BF16)
        incoming = incoming + dot(down_rows[:, t : t + 512], messages)
    new1 = node_update(level1[...], first, incoming.astype(BF16), up_in, up_out, up_gain)

    parents2 = packed_numbers(parent2[...], N2, R2)
    weights = flat_row(weight2)
    sums2[...] = spread_sums(new1, parents2 - N2, weights, 8 * R2).astype(BF16)
    small = R2 // PIECES
    send_sums = piecewise(2, small, lambda s, h: sums2.at[pl.ds(s * R2 + small * h, small)], land_c)
    send_rim = piecewise(3, small, lambda s, h: level2.at[pl.ds(small * h, small)], land_d)
    arriving = [send_sums(h) for h in range(PIECES)]
    spread = spread_sums(new1, parents2, weights, N2)
    level2[pl.ds(R2, N2 - R2), :] = spread[R2:].astype(BF16)
    moving = []
    for h in range(PIECES):
        finished(arriving[h])
        rim = spread[small * h : small * (h + 1)]
        for s in range(8):
            rim = rim + land_c[s, pl.ds(small * h, small)].astype(F32)
        level2[pl.ds(small * h, small), :] = rim.astype(BF16)
        moving = moving + send_rim(h)
    mine = dot(level2[...], msg_in[D:]).astype(BF16)
    own = dot(level2[...], msg_in[:D]).astype(BF16)
    numbers = packed_numbers(src2, N2, R2)
    pad = jnp.zeros((64, D), BF16)
    start = dot(pick_matrix(dst2, 0, E2, 128), jnp.concatenate([mine, pad], axis=0)) + dot(
        pick_matrix(numbers, 0, E2, 128), jnp.concatenate([own, pad], axis=0)
    )
    first = dot(level2[...], up_in[:D])
    finished(moving)
    beyond = dot(land_d[...].reshape(8 * R2, D), msg_in[:D]).astype(BF16)
    hidden = silu(start + dot(pick_matrix(numbers, 0, E2, 8 * R2, N2), beyond)).astype(BF16)
    messages = normed(dot(hidden, msg_out[...]), flat_row(msg_gain)).astype(BF16)
    incoming = dot(gather_sums(dst2, N2), messages).astype(BF16)
    new2[...] = node_update(level2[...], first, incoming, up_in, up_out, up_gain)

    moving = swap(4, lambda s: new2.at[pl.ds(0, R2)], land_e)
    numbers = packed_numbers(parent2[...], N2, R2)
    lift = new1.astype(F32) + dot(
        pick_matrix(numbers, 0, N1, 128), jnp.concatenate([new2[...], pad], axis=0)
    )
    finished(moving)
    final1[...] = (
        lift + dot(pick_matrix(numbers, 0, N1, 8 * R2, N2), land_e[...].reshape(8 * R2, D))
    ).astype(BF16)

    moving = swap(5, lambda s: final1.at[pl.ds(0, R1)], land_f)
    for t in range(0, NF, 512):
        preact[pl.ds(t, 512), :] = fine[pl.ds(t, 512), :].astype(F32) + dot(
            pick_matrix(parents, t, 512, N1), final1[...]
        )
    finished(moving)
    rims = land_f[...].reshape(8 * R1, D)
    for t in range(0, NF, 512):
        out[pl.ds(t, 512), :] = (
            preact[pl.ds(t, 512), :] + dot(pick_matrix(parents, t, 512, 8 * R1, N1), rims)
        ).astype(BF16)


LOADS = (
    "nodes", "bnd", "w_in", "dst", "src", "w_out", "gain", "up_in", "up_out", "up_gain",
    "parent1", "weight1", "src1", "dst1", "parent2", "weight2", "src2", "dst2",
    "msg_in", "msg_out", "msg_gain", "cup_in", "cup_out", "cup_gain",
)


def flat_row(ref):
    return ref[...].astype(F32).reshape(1, -1)


def block_kernel(n_gx, n_gy, *refs):
    count = len(LOADS)
    far = dict(zip(LOADS, refs[:count]))
    latent_far, out = refs[count], refs[count + 1]
    here = dict(zip(LOADS, refs[count + 2 : 2 * count + 2]))
    (
        latent, base, first, table, picked, picked_b, messages_a, messages_b, total, target, edge_rows, halo,
        fine, sums1, land_a, level1, land_b, sums2, land_c, level2, land_d, new2, land_e,
        final1, land_f, preact, load_sem, latent_sem, halo_send, halo_recv,
        send_sem, recv_sem, piece_send, piece_recv,
    ) = refs[2 * count + 2 :]
    around = neighbours(n_gx, n_gy)
    greet(around)
    loads = {
        name: pltpu.make_async_copy(far[name], here[name], load_sem.at[i])
        for i, name in enumerate(LOADS)
    }

    def latent_copy(i):
        part = pl.ds(pl.multiple_of(i * T1, T1), T1)
        return pltpu.make_async_copy(latent_far.at[part], latent.at[part], latent_sem.at[i])

    for name in ("nodes", "bnd", "w_in", "dst", "src"):
        loads[name].start()
    for i in range(EDGES // T1):
        latent_copy(i).start()
    for name in LOADS[5:]:
        loads[name].start()

    nodes, dst, w_in = here["nodes"], here["dst"], here["w_in"]
    for name in ("nodes", "bnd"):
        loads[name].wait()
    edge_rows[...] = dot(pick_rows(here["bnd"][...], NF), nodes[...]).astype(BF16)
    for name in ("w_in", "dst", "src"):
        loads[name].wait()
    target[...] = (0.5 * dot(nodes[...], w_in[D : 2 * D])).astype(BF16)

    def base_step(i, _):
        latent_copy(i).wait()
        part = pl.ds(pl.multiple_of(i * T1, T1), T1)
        base[part, :] = dot(pick_matrix(dst[i], 0, T1, NF), target[...]) + 0.5 * dot(
            latent[part, :], w_in[2 * D :]
        )
        return 0

    lax.fori_loop(0, EARLY, base_step, 0)
    all_greeted()
    halo_moving = exchange(around, lambda s: edge_rows, halo, halo_send, halo_recv)
    lax.fori_loop(EARLY, EDGES // T1, base_step, 0)

    def fill(rows, start):
        value = 0.5 * dot(rows, w_in[:D])
        table[pl.ds(start, 256)] = value.reshape(256, 4, 128)

    for c in range(0, NF, 256):
        fill(nodes[pl.ds(c, 256), :], c)
    total[...] = jnp.zeros_like(total)
    for name in LOADS[5:]:
        loads[name].wait()
    first[...] = dot(nodes[...], here["up_in"][:D])
    finished(halo_moving)
    for s in range(0, 8, 2):
        fill(halo[pl.ds(s, 2)].reshape(2 * BND, D), NF + BND * (s + s // 4))

    quarter = T2 // 4

    def pick(rows, i, t):
        for e in range(quarter * t, quarter * (t + 1)):
            rows[pl.ds(4 * e, 4), :] = table[here["src"][i * T2 + e]]

    def edge_sums(messages, i, t):
        numbers = jnp.concatenate(
            [dst[i * (T2 // T1) + u] for u in range(T2 // T1)], axis=1
        ) - NF // 4 * t
        part = pl.ds(NF // 4 * t, NF // 4)
        total[part, :] += dot(gather_sums(numbers, NF // 4), messages[...])

    def edge_group(i, rows, messages, next_rows, last_messages):
        last = jnp.maximum(i - 1, 0)
        following = jnp.minimum(i + 1, EDGES // T2 - 1)
        for t in range(4):
            part = pl.ds(pl.multiple_of(i * T2 + quarter * t, quarter), quarter)
            half = base[part, :] + jnp.concatenate(
                [rows[pl.ds(4 * quarter * t + j, quarter, stride=4), :] for j in range(4)],
                axis=1,
            )
            hidden = (half + half * jnp.tanh(half)).astype(BF16)
            pick(next_rows, following, t)
            messages[pl.ds(quarter * t, quarter), :] = normed(
                dot(hidden, here["w_out"][...])
            ).astype(BF16)
            edge_sums(last_messages, last, t)

    def edge_step(k, _):
        edge_group(2 * k, picked, messages_a, picked_b, messages_b)
        edge_group(2 * k + 1, picked_b, messages_b, picked, messages_a)
        return 0

    messages_b[...] = jnp.zeros_like(messages_b)
    for t in range(4):
        pick(picked, 0, t)
    lax.fori_loop(0, EDGES // T2 // 2, edge_step, 0)
    for t in range(4):
        edge_sums(messages_b, EDGES // T2 - 1, t)
    total[...] = total[...] * flat_row(here["gain"])
    fine[...] = node_update(
        nodes[...], first[...], total[...].astype(BF16), here["up_in"], here["up_out"], here["up_gain"]
    )

    coarse_part(
        around, fine, *[here[name] for name in LOADS[10:]], out,
        sums1, land_a, level1, land_b, sums2, land_c, level2, land_d, new2, land_e,
        final1, land_f, preact, send_sem, recv_sem, piece_send, piece_recv,
    )


def per_device(n_gx, n_gy, args):
    (
        fine_nodes, edge_latent, boundary, fine_src, fine_dst, parent_one, weight_one,
        coarse_src_one, coarse_dst_one, parent_two, weight_two, coarse_src_two, coarse_dst_two,
        fine_message_in, fine_message_out, fine_message_gain,
        fine_update_in, fine_update_out, fine_update_gain,
        coarse_message_in, coarse_message_out, coarse_message_gain,
        coarse_update_in, coarse_update_out, coarse_update_gain,
    ) = args

    def row(v):
        return v.reshape(1, -1)

    given = dict(
        nodes=fine_nodes, bnd=row(boundary), w_in=fine_message_in,
        dst=fine_dst.reshape(EDGES // T1, 1, T1), src=fine_src,
        w_out=fine_message_out, gain=fine_message_gain,
        up_in=fine_update_in, up_out=fine_update_out, up_gain=fine_update_gain,
        parent1=row(parent_one), weight1=weight_one,
        src1=coarse_src_one, dst1=coarse_dst_one,
        parent2=row(parent_two), weight2=weight_two,
        src2=coarse_src_two, dst2=coarse_dst_two,
        msg_in=coarse_message_in, msg_out=coarse_message_out, msg_gain=coarse_message_gain,
        cup_in=coarse_update_in, cup_out=coarse_update_out, cup_gain=coarse_update_gain,
    )
    operands = [given[name] for name in LOADS]
    return pl.pallas_call(
        lambda *refs: block_kernel(n_gx, n_gy, *refs),
        name="block",
        out_shape=jax.ShapeDtypeStruct((NF, D), BF16),
        in_specs=[pl.BlockSpec(memory_space=pltpu.HBM)] * (len(LOADS) + 1),
        out_specs=pl.BlockSpec(memory_space=pltpu.VMEM),
        scratch_shapes=[
            (pltpu.SMEM if name == "src" else pltpu.VMEM)(v.shape, v.dtype)
            for name, v in zip(LOADS, operands)
        ]
        + [
            pltpu.VMEM((EDGES, D), BF16),
            pltpu.VMEM((EDGES, D), F32),
            pltpu.VMEM((NF, D), F32),
            pltpu.VMEM((NF + 9 * BND, 4, 128), F32),
            pltpu.VMEM((T2 * 4, 128), F32),
            pltpu.VMEM((T2 * 4, 128), F32),
            pltpu.VMEM((T2, D), BF16),
            pltpu.VMEM((T2, D), BF16),
            pltpu.VMEM((NF, D), F32),
            pltpu.VMEM((NF, D), BF16),
            pltpu.VMEM((BND, D), BF16),
            pltpu.VMEM((8, BND, D), BF16),
            pltpu.VMEM((NF, D), BF16),
            pltpu.VMEM((8 * R1, D), BF16),
            pltpu.VMEM((8, R1, D), BF16),
            pltpu.VMEM((N1, D), BF16),
            pltpu.VMEM((8, R1, D), BF16),
            pltpu.VMEM((8 * R2, D), BF16),
            pltpu.VMEM((8, R2, D), BF16),
            pltpu.VMEM((N2, D), BF16),
            pltpu.VMEM((8, R2, D), BF16),
            pltpu.VMEM((N2, D), BF16),
            pltpu.VMEM((8, R2, D), BF16),
            pltpu.VMEM((N1, D), BF16),
            pltpu.VMEM((8, R1, D), BF16),
            pltpu.VMEM((E1, D), F32),
            pltpu.SemaphoreType.DMA((len(LOADS),)),
            pltpu.SemaphoreType.DMA((EDGES // T1,)),
            pltpu.SemaphoreType.DMA((8,)),
            pltpu.SemaphoreType.DMA((8,)),
            pltpu.SemaphoreType.DMA((6, 8)),
            pltpu.SemaphoreType.DMA((6, 8)),
            pltpu.SemaphoreType.DMA((4, PIECES, 8)),
            pltpu.SemaphoreType.DMA((4, PIECES, 8)),
        ],
        compiler_params=pltpu.CompilerParams(
            collective_id=0, has_side_effects=True, vmem_limit_bytes=58 * 2**20
        ),
    )(*operands, edge_latent)


def solution(mesh):
    both = ("gx", "gy")
    in_specs = (P(both, None), P(both, None)) + (P(both),) * 11 + (P(),) * 12
    return jax.shard_map(
        lambda *args: per_device(mesh.shape["gx"], mesh.shape["gy"], args),
        mesh=mesh,
        in_specs=in_specs,
        out_specs=P(both, None),
        check_vma=False,
    )
```
